512 devices in a mesh: graphs: 2 (over y), rows: 32 (over z), cols: 4 (over x), sub: 2 (over core).
Axes of the slice: x: 4, y: 2, z: 32, core: 2. Of those that a mesh axis runs over, the one named last changes fastest.
The devices are a block of a 4x8x32 slice.
Arguments:
- current_block: float32 [16, 1048576], P(None, ('graphs', 'rows', 'cols', 'sub')), parts along dimension 1, may hold values from -1200 to 1200, as said below
- previous_block: float32 [16, 1048576], P(None, ('graphs', 'rows', 'cols', 'sub')), parts along dimension 1, may hold values from -1200 to 1200, as said below
- adjacency_tiles: float32 [24576, 128, 128], P(('graphs', 'rows', 'cols', 'sub')), parts along dimension 0, may hold values from -0.3125 to 0.3125
- tile_rows: int32 [24576], P(('graphs', 'rows', 'cols', 'sub')), parts along dimension 0, may hold values from 0 to 4095, as said below
- tile_cols: int32 [24576], P(('graphs', 'rows', 'cols', 'sub')), parts along dimension 0, may hold values from 0 to 4095, as said below
- tile_count: int32 [512], P(('graphs', 'rows', 'cols', 'sub')), parts along dimension 0, may hold values from 18 to 48, as said below
- locked: int32 [2], P('graphs'), parts along dimension 0, may hold values from 0 to 7
Outputs:
- w_basis: float32 [16, 1048576], P(None, ('graphs', 'rows', 'cols', 'sub')), parts along dimension 1
- w_image: float32 [16, 1048576], P(None, ('graphs', 'rows', 'cols', 'sub')), parts along dimension 1
- ritz_matrix: float32 [96, 48], P('graphs'), parts along dimension 0
The draws below stay inside these ranges and needn't reach their ends.
There are 2 independent parts, one for each index of `graphs`. The reference program is written for one: setup_inputs(seed, part) draws one part's arguments, and reference() takes and returns one part's arrays. A program takes and returns all parts, laid end to end along the dimension named above; each array names one. Nothing has to cross between parts.
Inputs may be any that keep to these rules, and one draw needn't show every extreme that they name: `current_block`: entries of order one to some hundreds. `previous_block`: entries of order one to some hundreds. Slots d * 48 to (d + 1) * 48 - 1 belong to device d and name its own tile rows d * 16 to (d + 1) * 16 - 1. The first 16 slots of a device name its tile rows in order, with tile_cols equal to tile_rows. Slots past the device's count name tile row d * 16 and carry no weight. `tile_cols`: A slot of device d names a tile column from d * 16 - 8 to (d + 1) * 16 + 7. Slot 16 of a device names a tile of the block before it and slot 17 one of the block after it, where such a block exists. A pair of tile row and tile column may stand in several slots; their tiles add. `tile_count`: in every draw some device has all 48 slots live.
All inputs are finite; a program needn't handle non-finite values.
Results may differ from the reference program's by a relative error of at most 0.000094.
Values sent between devices are 32-bit elements; how exact they have to be, the bound alone decides.
A program may use at most 64 MiB of HBM per device.

```python
import jax
import jax.numpy as jnp
from jax import lax

K = 16
TILE_VERTICES = 128
DEVICE_SLOTS = 3
DEVS = 256
DEVICE_TILE_ROWS = 16
REACH = 8
MAXT_DEV = 48
NV = 524288
NT = 4096
GRAPH_SLOTS = 12288


def tile_arrangement(key):
    keys = jax.random.split(jax.random.fold_in(key, 11), 6)
    devices = jnp.arange(DEVS, dtype=jnp.int32)
    slot_indices = jnp.arange(MAXT_DEV, dtype=jnp.int32)[None, :]
    extra = jax.random.randint(keys[0], (DEVS,), 2, MAXT_DEV - DEVICE_TILE_ROWS + 1)
    fullest = jax.random.randint(keys[1], (), 0, DEVS)
    extra = jnp.where(devices == fullest, MAXT_DEV - DEVICE_TILE_ROWS, extra)
    counts = (DEVICE_TILE_ROWS + extra).astype(jnp.int32)
    row_offset = jax.random.randint(keys[2], (DEVS, MAXT_DEV), 0, DEVICE_TILE_ROWS)
    col_offset = jax.random.randint(keys[3], (DEVS, MAXT_DEV), -REACH, DEVICE_TILE_ROWS + REACH)
    left_offset = jax.random.randint(keys[4], (DEVS, MAXT_DEV), -REACH, 0)
    right_offset = DEVICE_TILE_ROWS + jax.random.randint(keys[5], (DEVS, MAXT_DEV), 0, REACH)
    col_offset = jnp.where(slot_indices == DEVICE_TILE_ROWS, left_offset, col_offset)
    col_offset = jnp.where(slot_indices == DEVICE_TILE_ROWS + 1, right_offset, col_offset)
    diagonal = slot_indices < DEVICE_TILE_ROWS
    row_offset = jnp.where(diagonal, slot_indices, row_offset)
    col_offset = jnp.where(diagonal, slot_indices, col_offset)
    padded = slot_indices >= counts[:, None]
    row_offset = jnp.where(padded, 0, row_offset)
    col_offset = jnp.where(padded, 0, col_offset)
    rows_out = devices[:, None] * DEVICE_TILE_ROWS + row_offset
    cols_out = devices[:, None] * DEVICE_TILE_ROWS + col_offset
    cols_out = jnp.where(cols_out < 0, cols_out + REACH, cols_out)
    cols_out = jnp.where(cols_out >= NT, cols_out - REACH, cols_out)
    return (rows_out.reshape(-1).astype(jnp.int32), cols_out.reshape(-1).astype(jnp.int32), counts)


def draw_tile_rows(key, part):
    return tile_arrangement(key)[0]


def draw_tile_cols(key, part):
    return tile_arrangement(key)[1]


def draw_tile_count(key, part):
    return tile_arrangement(key)[2]


def draw_locked(key, part):
    base = jax.random.randint(jax.random.fold_in(key, 53), (1,), 0, 7)
    return jnp.where(part % 2 == 1, 7, base).astype(jnp.int32)


def vector_draw(key):
    keys = jax.random.split(key, 4)
    where_along = jnp.arange(NV, dtype=jnp.float32) / NV
    rising = jnp.sqrt(1.0 + 2.0 * where_along)
    base = jax.random.truncated_normal(keys[0], -5.0, 5.0, (K, NV), jnp.float32)
    rough = 10.0 ** jax.random.uniform(keys[2], (NV,), jnp.float32)
    column_scale = 10.0 ** jax.random.uniform(keys[3], (K,), jnp.float32)
    return base * (rough * rising)[None, :] * column_scale[:, None]


def draw_current_block(key, part):
    return vector_draw(jax.random.fold_in(key, 21))


def draw_previous_block(key, part):
    return vector_draw(jax.random.fold_in(key, 37))


def shard_levels(rng, dims, cuts, smallest, high):
    loudness = 1.0
    for dim, blocks in cuts:
        draws = jax.random.uniform(jax.random.fold_in(jax.random.fold_in(rng, 6), dim), (blocks,), jnp.float32, smallest / len(cuts), high / len(cuts))
        loudness = loudness * jnp.repeat(jnp.exp(draws), dims[dim] // blocks).reshape((-1,) + (1,) * (len(dims) - 1 - dim))
    return loudness


def normal_values(rng, dims, spread, most, shards=(), kind=jnp.bfloat16):
    drawn = spread * jax.random.normal(rng, dims, jnp.float32)
    if shards:
        drawn = drawn * shard_levels(rng, dims, shards, -0.22, 0.18)
    return jnp.clip(drawn, -most, most).astype(kind)


def setup_inputs(seed: int = 0, part: int = 0) -> dict:
    splits = jax.random.split(jax.random.key(seed), 8)
    own_keys = jax.random.split(jax.random.fold_in(splits[7], part), 8)
    return {
        "current_block": draw_current_block(jax.random.fold_in(jax.random.fold_in(splits[7], part), 71), part),
        "previous_block": draw_previous_block(jax.random.fold_in(jax.random.fold_in(splits[7], part), 71), part),
        "adjacency_tiles": normal_values(own_keys[2], (GRAPH_SLOTS, TILE_VERTICES, TILE_VERTICES), (DEVICE_SLOTS * TILE_VERTICES) ** -0.5, 0.3125, ((0, 256),), jnp.float32),
        "tile_rows": draw_tile_rows(jax.random.fold_in(jax.random.fold_in(splits[7], part), 71), part),
        "tile_cols": draw_tile_cols(jax.random.fold_in(jax.random.fold_in(splits[7], part), 71), part),
        "tile_count": draw_tile_count(jax.random.fold_in(jax.random.fold_in(splits[7], part), 71), part),
        "locked": draw_locked(jax.random.fold_in(jax.random.fold_in(splits[7], part), 71), part),
    }


def apply_operator(vectors, adjacency_tiles, tile_rows, tile_cols, live_mask):
    channels = vectors.shape[0]
    column_blocks = vectors.reshape(channels, NT, TILE_VERTICES)
    gathered = jnp.take(column_blocks, tile_cols, axis=1)
    products = jnp.einsum('cta,tab->tcb', gathered, adjacency_tiles, precision=lax.Precision.HIGHEST)
    products = products * live_mask[:, None, None]
    summed = jax.ops.segment_sum(products, tile_rows, num_segments=NT)
    return vectors - jnp.transpose(summed, (1, 0, 2)).reshape(channels, NV)

def inner_products(left, right):
    return jnp.dot(left, right.T, precision=lax.Precision.HIGHEST)

def rayleigh_ritz(gram_b, gram_a):
    factor_b = jnp.linalg.cholesky(gram_b)
    symmetric = 0.5 * (gram_a + gram_a.T)
    halfway = lax.linalg.triangular_solve(factor_b, symmetric, left_side=True, lower=True)
    return lax.linalg.triangular_solve(factor_b, halfway.T, left_side=True, lower=True)

def reference(current_block, previous_block, adjacency_tiles, tile_rows, tile_cols, tile_count, locked):
    slot_indices = jnp.arange(GRAPH_SLOTS, dtype=jnp.int32)
    owners = slot_indices // MAXT_DEV
    live_mask = (slot_indices % MAXT_DEV < tile_count[owners]).astype(jnp.float32)
    stacked = jnp.concatenate([current_block, previous_block], axis=0)
    images = apply_operator(stacked, adjacency_tiles, tile_rows, tile_cols, live_mask)
    x_image = images[:K]
    p_image = images[K:]
    quotient = jnp.sum(current_block * x_image, axis=1) / (jnp.sum(current_block * current_block, axis=1) + 1e-06)
    frozen_rows = jnp.arange(K, dtype=jnp.int32) < locked[0]
    residual = jnp.where(frozen_rows[:, None], 0.0, x_image - quotient[:, None] * current_block)
    gram_w = inner_products(residual, residual) / NV + jnp.diag(frozen_rows.astype(jnp.float32))
    factor = jnp.linalg.cholesky(gram_w)
    w_basis = lax.linalg.triangular_solve(factor, residual, left_side=True, lower=True)
    w_image = apply_operator(w_basis, adjacency_tiles, tile_rows, tile_cols, live_mask)
    search = jnp.concatenate([current_block, w_basis, previous_block], axis=0)
    search_image = jnp.concatenate([x_image, w_image, p_image], axis=0)
    zero_rows = jnp.zeros((K,), jnp.float32)
    pad_diag = jnp.concatenate([zero_rows, frozen_rows.astype(jnp.float32), zero_rows])
    gram_b = inner_products(search, search) / NV + jnp.diag(pad_diag)
    gram_a = inner_products(search, search_image) / NV
    ritz_matrix = rayleigh_ritz(gram_b, gram_a)
    return (w_basis, w_image, ritz_matrix)
```

```python
import functools

import jax
import jax.numpy as jnp
from jax import lax
from jax.experimental import pallas as pl
from jax.experimental.pallas import tpu as pltpu
from jax.sharding import PartitionSpec as P

MESH = pl.DeviceIdType.MESH
F32 = jnp.float32
BF16 = jnp.bfloat16
VMEM = pltpu.VMEM
VERTEX_AXES = ("rows", "cols", "sub")
CHUNKS = 4
GROUP = 8
PACKED = 32


def halves(value):
    high = value.astype(BF16)
    return high, (value - high.astype(F32)).astype(BF16)


def fill_tiles(split, first, value):
    width = split.shape[2]
    for i in range(value.shape[1] // width):
        split[first + i] = jnp.concatenate(halves(value[:, i * width : (i + 1) * width]), axis=0)


def tile_copies(tiles_ref, tiles, sems):
    each = tiles.shape[0] // CHUNKS
    return [
        pltpu.make_async_copy(
            tiles_ref.at[pl.ds(i * each, each)], tiles.at[pl.ds(i * each, each)], sems.at[i]
        )
        for i in range(CHUNKS)
    ]


def slot_product(left, tile):
    channels = left.shape[0] // 2
    high, low = halves(tile)
    both = jnp.concatenate([high, low], axis=1)
    out = jnp.dot(left, both, preferred_element_type=F32)
    width = tile.shape[1]
    top, bottom = out[:channels], out[channels:]
    return (top[:, :width] + (top[:, width:] + bottom[:, :width])) + bottom[:, width:]


def products(split, tiles, prods, first, last, column):
    def step(block, carry):
        for lane in range(GROUP):
            slot = block * GROUP + lane
            prods[slot] = slot_product(split[column(slot)], tiles[slot])
        return carry

    lax.fori_loop(first // GROUP, last // GROUP, step, 0)


def summed_rows(prods, rows_s, count_s, base, row_tiles, store):
    slots = prods.shape[0]
    count = count_s[0]
    for block in range(row_tiles // 4):
        mine = [block * 4 + i for i in range(4)]

        def step(slot, sums):
            value = prods[slot]
            row = rows_s[slot] - base
            live = jnp.clip(count - slot, 0, 1)
            return tuple(
                s + (live * (1 - jnp.minimum(jnp.abs(row - i), 1))).astype(F32) * value
                for i, s in zip(mine, sums)
            )

        sums = lax.fori_loop(
            row_tiles, slots, step, tuple(prods[i] for i in mine), unroll=8
        )
        for i, s in zip(mine, sums):
            store(i, s)


def place(sizes):
    rows, cols, sub = (lax.axis_index(a) for a in VERTEX_AXES)
    return (rows * sizes[1] + cols) * sizes[2] + sub


def device_at(position, sizes):
    return {
        "rows": position // (sizes[1] * sizes[2]),
        "cols": (position // sizes[2]) % sizes[1],
        "sub": position % sizes[2],
    }


def first_kernel(
    sizes, x, p, tiles_ref, rows_s, cols_s, count_s, yext, q,
    tiles, wide, split, ywide, prods, tile_sems, send, recv,
):
    channels, here = x.shape
    width = tiles.shape[1]
    row_tiles = here // width
    reach = here // 2
    total = sizes[0] * sizes[1] * sizes[2]
    me = place(sizes)
    base = me * row_tiles
    loads = tile_copies(tiles_ref, tiles, tile_sems)
    for load in loads:
        load.start()
    has_low, has_high = me > 0, me < total - 1
    low, high = device_at(me - 1, sizes), device_at(me + 1, sizes)
    barrier = pltpu.get_barrier_semaphore()

    @pl.when(has_low)
    def _():
        pl.semaphore_signal(barrier, inc=1, device_id=low, device_id_type=MESH)

    @pl.when(has_high)
    def _():
        pl.semaphore_signal(barrier, inc=1, device_id=high, device_id_type=MESH)

    pl.semaphore_wait(barrier, has_low.astype(jnp.int32) + has_high.astype(jnp.int32))

    def remote(source, target, n, device):
        return pltpu.make_async_remote_copy(
            src_ref=source, dst_ref=target, send_sem=send.at[n], recv_sem=recv.at[n],
            device_id=device, device_id_type=MESH,
        )

    own = pl.ds(reach, here)
    low_side, high_side = pl.ds(0, reach), pl.ds(reach + here, reach)
    to_low = [
        remote(v.at[:, pl.ds(0, reach)], wide.at[pl.ds(i * channels, channels), high_side], i, low)
        for i, v in enumerate((x, p))
    ]
    to_high = [
        remote(
            v.at[:, pl.ds(here - reach, reach)],
            wide.at[pl.ds(i * channels, channels), low_side], 2 + i, high,
        )
        for i, v in enumerate((x, p))
    ]
    y_low = remote(ywide.at[:, pl.ds(reach, reach)], ywide.at[:, high_side], 4, low)
    y_high = remote(ywide.at[:, pl.ds(here, reach)], ywide.at[:, low_side], 5, high)

    @pl.when(has_low)
    def _():
        for copy in to_low:
            copy.start()

    @pl.when(has_high)
    def _():
        for copy in to_high:
            copy.start()

    def fill(first, value):
        fill_tiles(split, first, value)

    reach_tiles = reach // width
    fill(reach_tiles, jnp.concatenate([x[...], p[...]], axis=0))
    loads[0].wait()
    loads[1].wait()
    products(split, tiles, prods, 0, row_tiles, lambda slot: slot + reach_tiles)

    @pl.when(has_low)
    def _():
        for copy in to_low:
            copy.wait_send()
        for copy in to_high:
            copy.wait_recv()

    @pl.when(has_high)
    def _():
        for copy in to_high:
            copy.wait_send()
        for copy in to_low:
            copy.wait_recv()

    @pl.when(jnp.logical_not(has_low))
    def _():
        wide[:, low_side] = jnp.zeros((2 * channels, reach), F32)
        ywide[:, low_side] = jnp.zeros((channels, reach), F32)

    @pl.when(jnp.logical_not(has_high))
    def _():
        wide[:, high_side] = jnp.zeros((2 * channels, reach), F32)
        ywide[:, high_side] = jnp.zeros((channels, reach), F32)

    fill(0, wide[:, low_side])
    fill(reach_tiles + row_tiles, wide[:, high_side])
    for load in loads[2:]:
        load.wait()
    products(
        split, tiles, prods, row_tiles, tiles.shape[0],
        lambda slot: jnp.clip(cols_s[slot] - (base - reach_tiles), 0, split.shape[0] - 1),
    )

    def store(i, value):
        ywide[:, pl.ds(reach + i * width, width)] = value[:channels]
        q[:, pl.ds(i * width, width)] = value[channels:]

    summed_rows(prods, rows_s, count_s, base, row_tiles, store)

    @pl.when(has_low)
    def _():
        y_low.start()

    @pl.when(has_high)
    def _():
        y_high.start()

    yext[:, own] = ywide[:, own]

    @pl.when(has_low)
    def _():
        y_low.wait_send()
        y_high.wait_recv()

    @pl.when(has_high)
    def _():
        y_high.wait_send()
        y_low.wait_recv()

    yext[:, low_side] = ywide[:, low_side]
    yext[:, high_side] = ywide[:, high_side]


def second_kernel(
    sizes, x, p, q, yext, tiles_ref, rows_s, cols_s, count_s, total_ref, z,
    tiles, split, prods, parts, arrived, along, gathered, tile_sems,
    send_a, recv_a, send_b, recv_b, send_c, recv_c,
):
    channels, here = x.shape
    width = tiles.shape[1]
    row_tiles = here // width
    reach = here // 2
    reach_tiles = reach // width
    depth, cols, sub = sizes
    members = cols * sub
    me = place(sizes)
    base = me * row_tiles
    layer = lax.axis_index("rows")
    member = lax.axis_index("cols") * sub + lax.axis_index("sub")
    barrier = pltpu.get_barrier_semaphore()
    loads = tile_copies(tiles_ref, tiles, tile_sems)
    for load in loads:
        load.start()

    def layer_at(k):
        half = (k + 1) // 2
        offset = jnp.where(k % 2 == 1, half, -half)
        return (layer + depth // 2 + depth + offset) % depth

    def member_at(k):
        other = (member + k + 1) % members
        return other, {"cols": other // sub, "sub": other % sub}

    def greet_layer(k, carry):
        pl.semaphore_signal(barrier, inc=1, device_id={"rows": layer_at(k)}, device_id_type=MESH)
        return carry

    def greet_member(k, carry):
        pl.semaphore_signal(barrier, inc=1, device_id=member_at(k)[1], device_id_type=MESH)
        return carry

    lax.fori_loop(0, depth - 1, greet_layer, 0)
    lax.fori_loop(0, members - 1, greet_member, 0)

    fill_tiles(split, 0, yext[...])
    for load in loads:
        load.wait()
    products(split, tiles, prods, 0, row_tiles, lambda slot: slot + reach_tiles)
    products(
        split, tiles, prods, row_tiles, tiles.shape[0],
        lambda slot: jnp.clip(cols_s[slot] - (base - reach_tiles), 0, split.shape[0] - 1),
    )

    def store(i, value):
        z[:, pl.ds(i * width, width)] = value

    summed_rows(prods, rows_s, count_s, base, row_tiles, store)

    xs, ps = x[...], p[...]
    ys = yext[:, pl.ds(reach, here)]
    left = jnp.concatenate([xs, ys, ps], axis=0)
    right = jnp.concatenate([xs, ys, z[...], ps, q[...]], axis=0)
    right = jnp.concatenate([right, jnp.zeros((128 - 5 * channels, here), F32)], axis=0)
    gram = lax.dot_general(
        left, right, (((1,), (1,)), ((), ())), precision=lax.Precision.HIGHEST,
        preferred_element_type=F32,
    )
    lane = lax.broadcasted_iota(jnp.int32, (channels, 128), 1)
    turned = pltpu.roll(gram[2 * channels :], 3 * channels, 1)
    packed = jnp.concatenate(
        [jnp.where(lane < 5 * channels, gram[:channels], turned), gram[channels : 2 * channels]],
        axis=0,
    )
    rows_each = PACKED // members
    for i in range(members):
        parts[i] = packed[i * rows_each : (i + 1) * rows_each]

    pl.semaphore_wait(barrier, depth - 1 + members - 1)

    def spread(k):
        other, device = member_at(k)
        return pltpu.make_async_remote_copy(
            src_ref=parts.at[other], dst_ref=arrived.at[member], send_sem=send_a.at[other],
            recv_sem=recv_a.at[member], device_id=device, device_id_type=MESH,
        )

    def spread_in(k):
        other, device = member_at(k)
        return pltpu.make_async_remote_copy(
            src_ref=parts.at[other], dst_ref=arrived.at[other], send_sem=send_a.at[other],
            recv_sem=recv_a.at[other], device_id=device, device_id_type=MESH,
        )

    def over(k):
        other = layer_at(k)
        return pltpu.make_async_remote_copy(
            src_ref=along.at[layer], dst_ref=along.at[layer], send_sem=send_b.at[other],
            recv_sem=recv_b.at[layer], device_id={"rows": other}, device_id_type=MESH,
        )

    def over_in(k):
        other = layer_at(k)
        return pltpu.make_async_remote_copy(
            src_ref=along.at[layer], dst_ref=along.at[other], send_sem=send_b.at[other],
            recv_sem=recv_b.at[other], device_id={"rows": other}, device_id_type=MESH,
        )

    def share(k):
        other, device = member_at(k)
        return pltpu.make_async_remote_copy(
            src_ref=gathered.at[member], dst_ref=gathered.at[member], send_sem=send_c.at[other],
            recv_sem=recv_c.at[member], device_id=device, device_id_type=MESH,
        )

    def share_in(k):
        other, device = member_at(k)
        return pltpu.make_async_remote_copy(
            src_ref=gathered.at[member], dst_ref=gathered.at[other], send_sem=send_c.at[other],
            recv_sem=recv_c.at[other], device_id=device, device_id_type=MESH,
        )

    def each(n, act):
        def step(k, carry):
            act(k)
            return carry

        lax.fori_loop(0, n, step, 0)

    each(members - 1, lambda k: spread(k).start())
    arrived[member] = parts[member]
    each(members - 1, lambda k: spread_in(k).wait_recv())
    along[layer] = jnp.sum(arrived[...], axis=0)
    each(depth - 1, lambda k: over(k).start())
    each(depth - 1, lambda k: over_in(k).wait_recv())
    gathered[member] = jnp.sum(along[...], axis=0)
    each(members - 1, lambda k: share(k).start())
    each(members - 1, lambda k: share_in(k).wait_recv())
    total_ref[...] = gathered[...]
    each(members - 1, lambda k: spread(k).wait_send())
    each(depth - 1, lambda k: over(k).wait_send())
    each(members - 1, lambda k: share(k).wait_send())


def eliminated(matrix):
    n = matrix.shape[0]
    row = lax.broadcasted_iota(jnp.int32, (n, 1), 0)
    pivots = []
    for k in range(n):
        top = matrix[k : k + 1]
        pivot = top[:, k : k + 1]
        pivots.append(pivot)
        if k < n - 1:
            scaled = top * (1.0 / pivot)
            matrix = matrix - jnp.where(row > k, matrix[:, k : k + 1], 0.0) * scaled
    return matrix * lax.rsqrt(jnp.concatenate(pivots, axis=0))


def precise(left, right, turned=False):
    return lax.dot_general(
        left, right, (((1,), (1 if turned else 0,)), ((), ())),
        precision=lax.Precision.HIGHEST, preferred_element_type=F32,
    )


def third_kernel(vertex_total, total_ref, x, yext, z, locked_s, w, w_image, ritz):
    channels, here = x.shape
    reach = here // 2
    packed = jnp.concatenate([total_ref[i] for i in range(total_ref.shape[0])], axis=0)
    first, second = packed[:channels], packed[channels:]

    def part(v, i):
        return v[:, i * channels : (i + 1) * channels]

    xx, xy, xz, xp, xq = (part(first, i) for i in range(5))
    pz, pp, pq = (part(first, i) for i in range(5, 8))
    yp = part(second, 3)
    shape = (channels, channels)
    row = lax.broadcasted_iota(jnp.int32, shape, 0)
    column = lax.broadcasted_iota(jnp.int32, shape, 1)
    eye = jnp.where(row == column, 1.0, 0.0).astype(F32)
    locked = locked_s[0]
    top = eye * (xy + 1e-06)
    below = eye * (xx + 1e-06)
    c_down = jnp.sum(top, axis=1, keepdims=True) / jnp.sum(below, axis=1, keepdims=True)
    c_along = jnp.sum(top, axis=0, keepdims=True) / jnp.sum(below, axis=0, keepdims=True)
    free_down = (lax.broadcasted_iota(jnp.int32, (channels, 1), 0) >= locked).astype(F32)
    free_along = (lax.broadcasted_iota(jnp.int32, (1, channels), 1) >= locked).astype(F32)
    scale = 1.0 / vertex_total
    frozen = eye * (1.0 - free_down)
    rd = free_down * (c_down * first - second)
    rx, ry = part(rd, 0), part(rd, 1)
    gram_w = free_along * (rx * c_along - ry) * scale + frozen
    inverse = eliminated(jnp.concatenate([gram_w, eye], axis=1))[:, channels:]

    xs, ys, zs = x[...], yext[:, pl.ds(reach, here)], z[...]
    r = free_down * (c_down * xs - ys)
    nr = free_down * (c_down * ys - zs)
    w[...] = precise(inverse, r)
    w_image[...] = precise(inverse, r - nr)

    wd = precise(inverse, rd)
    wx, wy, wz, wp, wq = (part(wd, i) for i in range(5))
    px, py = xp.T, yp.T

    def against_r(vx, vy):
        return free_along * (vx * c_along - vy)

    def against_image(vx, vy, vz):
        return free_along * (c_along * (vx - vy) - vy + vz)

    stacked = jnp.concatenate(
        [against_r(wx, wy), against_image(xx, xy, xz), against_image(wx, wy, wz),
         against_image(px, py, pz)], axis=0,
    )
    stacked = precise(stacked, inverse, turned=True)
    ww, xaw, waw, paw = (stacked[i * channels : (i + 1) * channels] for i in range(4))
    gram_b = jnp.concatenate(
        [
            jnp.concatenate([xx, wx.T, xp], axis=1) * scale,
            jnp.concatenate([wx * scale, ww * scale + frozen, wp * scale], axis=1),
            jnp.concatenate([px, wp.T, pp], axis=1) * scale,
        ], axis=0,
    )
    gram_a = jnp.concatenate(
        [
            jnp.concatenate([xx - xy, xaw, xp - xq], axis=1),
            jnp.concatenate([wx - wy, waw, wp - wq], axis=1),
            jnp.concatenate([px - py, paw, pp - pq], axis=1),
        ], axis=0,
    ) * scale
    n = 3 * channels
    big = (
        lax.broadcasted_iota(jnp.int32, (n, n), 0) == lax.broadcasted_iota(jnp.int32, (n, n), 1)
    ).astype(F32)
    lower = eliminated(jnp.concatenate([gram_b, big], axis=1))[:, n:]
    symmetric = 0.5 * (gram_a + gram_a.T)
    ritz[...] = precise(precise(lower, symmetric), lower, turned=True)


def body(sizes, current_block, previous_block, adjacency_tiles, tile_rows, tile_cols, tile_count, locked):
    channels, here = current_block.shape
    slots, width, _ = adjacency_tiles.shape
    depth, cols, sub = sizes
    members = cols * sub
    rows_each = PACKED // members
    vmem = pl.BlockSpec(memory_space=pltpu.VMEM)
    smem = pl.BlockSpec(memory_space=pltpu.SMEM)
    anywhere = pl.BlockSpec(memory_space=pl.ANY)
    dma = pltpu.SemaphoreType.DMA

    def like(*shape):
        return jax.ShapeDtypeStruct(shape, F32)

    yext, q = pl.pallas_call(
        functools.partial(first_kernel, sizes),
        name="first",
        out_shape=(like(channels, 2 * here), like(channels, here)),
        in_specs=[vmem, vmem, anywhere, smem, smem, smem],
        out_specs=(vmem, vmem),
        scratch_shapes=[
            VMEM((slots, width, width), F32),
            VMEM((2 * channels, 2 * here), F32),
            VMEM((2 * here // width, 4 * channels, width), BF16),
            VMEM((channels, 2 * here), F32),
            VMEM((slots, 2 * channels, width), F32),
            dma((CHUNKS,)), dma((6,)), dma((6,)),
        ],
        compiler_params=pltpu.CompilerParams(collective_id=0, has_side_effects=True),
    )(current_block, previous_block, adjacency_tiles, tile_rows, tile_cols, tile_count)
    total, z = pl.pallas_call(
        functools.partial(second_kernel, sizes),
        name="second",
        out_shape=(like(members, rows_each, 128), like(channels, here)),
        in_specs=[vmem, vmem, vmem, vmem, anywhere, smem, smem, smem],
        out_specs=(vmem, vmem),
        scratch_shapes=[
            VMEM((slots, width, width), F32),
            VMEM((2 * here // width, 2 * channels, width), BF16),
            VMEM((slots, channels, width), F32),
            VMEM((members, rows_each, 128), F32),
            VMEM((members, rows_each, 128), F32),
            VMEM((depth, rows_each, 128), F32),
            VMEM((members, rows_each, 128), F32),
            dma((CHUNKS,)),
            dma((members,)), dma((members,)),
            dma((depth,)), dma((depth,)),
            dma((members,)), dma((members,)),
        ],
        compiler_params=pltpu.CompilerParams(collective_id=1, has_side_effects=True),
    )(current_block, previous_block, q, yext, adjacency_tiles, tile_rows, tile_cols, tile_count)
    vertex_total = here * depth * members
    return pl.pallas_call(
        functools.partial(third_kernel, float(vertex_total)),
        name="third",
        out_shape=(like(channels, here), like(channels, here), like(3 * channels, 3 * channels)),
        in_specs=[vmem, vmem, vmem, vmem, smem],
        out_specs=(vmem, vmem, vmem),
    )(total, current_block, yext, z, locked)


def solution(mesh):
    sizes = tuple(mesh.shape[a] for a in VERTEX_AXES)
    everywhere = ("graphs", "rows", "cols", "sub")
    in_specs = (
        P(None, everywhere),
        P(None, everywhere),
        P(everywhere, None, None),
        P(everywhere),
        P(everywhere),
        P(everywhere),
        P("graphs"),
    )
    out_specs = (P(None, everywhere), P(None, everywhere), P("graphs", None))
    return jax.shard_map(
        functools.partial(body, sizes), mesh=mesh, in_specs=in_specs, out_specs=out_specs,
        check_vma=False,
    )
```

```python
import functools

import jax
import jax.numpy as jnp
from jax import lax
from jax.experimental import pallas as pl
from jax.experimental.pallas import tpu as pltpu
from jax.sharding import PartitionSpec as P

MESH = pl.DeviceIdType.MESH
F32 = jnp.float32
BF16 = jnp.bfloat16
VMEM = pltpu.VMEM
VERTEX_AXES = ("rows", "cols", "sub")
CHUNKS = 4
GROUP = 8
PACKED = 24


def halves(value):
    high = value.astype(BF16)
    return high, (value - high.astype(F32)).astype(BF16)


def tile_copies(tiles_ref, tiles, sems):
    each = tiles.shape[0] // CHUNKS
    return [
        pltpu.make_async_copy(
            tiles_ref.at[pl.ds(i * each, each)], tiles.at[pl.ds(i * each, each)], sems.at[i]
        )
        for i in range(CHUNKS)
    ]


def fill_tiles(split, first, value):
    width = split.shape[2]
    for i in range(value.shape[1] // width):
        split[first + i] = jnp.concatenate(halves(value[:, i * width : (i + 1) * width]), axis=0)


def split_tiles(tiles, pairs, first, last):
    def step(block, carry):
        for lane in range(GROUP // 2):
            slot = block * (GROUP // 2) + lane
            pairs[slot] = jnp.concatenate(halves(tiles[slot]), axis=1)
        return carry

    lax.fori_loop(first // (GROUP // 2), last // (GROUP // 2), step, 0)


def products(split, pairs, prods, first, last, column):
    width = pairs.shape[1]
    channels = split.shape[1] // 2

    def step(block, carry):
        for lane in range(GROUP):
            slot = block * GROUP + lane
            out = jnp.dot(split[column(slot)], pairs[slot], preferred_element_type=F32)
            top, bottom = out[:channels], out[channels:]
            prods[slot] = (
                top[:, :width] + (top[:, width:] + bottom[:, :width])
            ) + bottom[:, width:]
        return carry

    lax.fori_loop(first // GROUP, last // GROUP, step, 0)


def summed_rows(prods, codes, row_tiles, store):
    slots, channels, width = prods.shape
    size = row_tiles // 2
    for block in range(2):
        mine = [block * size + i for i in range(size)]

        def step(slot, sums):
            value = prods[slot]
            row = jnp.full((channels, width), codes[slot], jnp.int32)
            return tuple(s + jnp.where(row == i, value, 0.0) for i, s in zip(mine, sums))

        sums = lax.fori_loop(
            row_tiles, slots, step, tuple(prods[i] for i in mine), unroll=4
        )
        for i, s in zip(mine, sums):
            store(i, s)


def place(sizes):
    rows, cols, sub = (lax.axis_index(a) for a in VERTEX_AXES)
    return (rows * sizes[1] + cols) * sizes[2] + sub


def device_at(position, sizes):
    return {
        "rows": position // (sizes[1] * sizes[2]),
        "cols": (position // sizes[2]) % sizes[1],
        "sub": position % sizes[2],
    }


def main_kernel(
    sizes, x_any, p_any, tiles_any, rows_any, cols_any, count_any, total_ref, y_any, z_any,
    xw, pw, yw, sx, sp, sy, tiles, pairs, prods, q, z, parts, arrived, along, gathered,
    rows_s, cols_s, count_s, codes, load_sems, tile_sems, halo_send, halo_recv,
    send_a, recv_a, send_b, recv_b, send_c, recv_c, out_sems, middle, far,
):
    channels, here = q.shape
    slots, width, _ = tiles.shape
    row_tiles = here // width
    reach = here // 2
    reach_tiles = reach // width
    depth, cols, sub = sizes
    members = cols * sub
    total = depth * members
    me = place(sizes)
    base = me * row_tiles
    layer = lax.axis_index("rows")
    member = lax.axis_index("cols") * sub + lax.axis_index("sub")
    near = depth // 8
    own = pl.ds(reach, here)
    low_side, high_side = pl.ds(0, reach), pl.ds(reach + here, reach)

    def layer_by(offset):
        other = layer + offset
        other = jnp.where(other >= depth, other - depth, other)
        return jnp.where(other < 0, other + depth, other)

    def layer_at(k):
        half = (k + 1) // 2
        return layer_by(depth // 2 + jnp.where(k % 2 == 1, half, -half))

    def member_by(offset):
        other = member + offset
        other = jnp.where(other >= members, other - members, other)
        return other, {"cols": other // sub, "sub": other % sub}

    def each(n, act):
        def step(k, carry):
            act(k)
            return carry

        lax.fori_loop(0, n, step, 0)

    barrier = pltpu.get_barrier_semaphore()

    def greet(semaphore, device):
        pl.semaphore_signal(semaphore, inc=1, device_id=device, device_id_type=MESH)

    has_low, has_high = me > 0, me < total - 1
    low, high = device_at(me - 1, sizes), device_at(me + 1, sizes)

    @pl.when(has_low)
    def _():
        greet(barrier, low)

    @pl.when(has_high)
    def _():
        greet(barrier, high)

    load_x = pltpu.make_async_copy(x_any, xw.at[:, own], load_sems.at[0])
    load_p = pltpu.make_async_copy(p_any, pw.at[:, own], load_sems.at[1])
    small = [
        pltpu.make_async_copy(source, target, load_sems.at[2 + i])
        for i, (source, target) in enumerate(
            ((rows_any, rows_s), (cols_any, cols_s), (count_any, count_s))
        )
    ]
    loads = tile_copies(tiles_any, tiles, tile_sems)
    for load in [load_x, load_p, *small, *loads]:
        load.start()
    for offset in range(1, members):
        greet(barrier, member_by(offset)[1])
    for offset in range(1, near + 1):
        greet(barrier, {"rows": layer_by(offset)})
        greet(barrier, {"rows": layer_by(-offset)})
    pl.semaphore_wait(
        barrier,
        has_low.astype(jnp.int32) + has_high.astype(jnp.int32) + (members - 1 + 2 * near),
    )

    def halo(wide, n):
        def remote(source, target, k, device):
            return pltpu.make_async_remote_copy(
                src_ref=wide.at[:, source], dst_ref=wide.at[:, target],
                send_sem=halo_send.at[k], recv_sem=halo_recv.at[k],
                device_id=device, device_id_type=MESH,
            )

        down = remote(pl.ds(reach, reach), high_side, 2 * n, low)
        up = remote(pl.ds(here, reach), low_side, 2 * n + 1, high)

        def start():
            @pl.when(has_low)
            def _():
                down.start()

            @pl.when(has_high)
            def _():
                up.start()

        def arrive():
            @pl.when(has_low)
            def _():
                up.wait_recv()

            @pl.when(has_high)
            def _():
                down.wait_recv()

        def finish():
            @pl.when(has_low)
            def _():
                down.wait_send()

            @pl.when(has_high)
            def _():
                up.wait_send()

        return start, arrive, finish

    x_start, x_arrive, x_finish = halo(xw, 0)
    p_start, p_arrive, p_finish = halo(pw, 1)
    y_start, y_arrive, y_finish = halo(yw, 2)

    load_x.wait()
    x_start()
    load_p.wait()
    p_start()
    greet(middle, {"rows": layer_by(near)})
    greet(middle, {"rows": layer_by(-near)})

    @pl.when(jnp.logical_not(has_low))
    def _():
        for wide in (xw, pw, yw):
            wide[:, low_side] = jnp.zeros((channels, reach), F32)

    @pl.when(jnp.logical_not(has_high))
    def _():
        for wide in (xw, pw, yw):
            wide[:, high_side] = jnp.zeros((channels, reach), F32)

    for load in small:
        load.wait()
    count = count_s[0]

    def code(slot):
        codes[slot] = jnp.where(slot < count, rows_s[slot] - base, -1)

    each(slots, code)

    def column(slot):
        return jnp.clip(cols_s[slot] - (base - reach_tiles), 0, 2 * row_tiles - 1)

    def inner(split):
        products(split, pairs, prods, 0, row_tiles, lambda slot: slot + reach_tiles)

    def outer(split):
        products(split, pairs, prods, row_tiles, slots, column)

    def fill_own(split, wide):
        fill_tiles(split, reach_tiles, wide[:, own])

    def fill_sides(split, wide):
        fill_tiles(split, 0, wide[:, low_side])
        fill_tiles(split, reach_tiles + row_tiles, wide[:, high_side])

    fill_own(sx, xw)
    for i, load in enumerate(loads):
        load.wait()
        split_tiles(tiles, pairs, i * slots // CHUNKS, (i + 1) * slots // CHUNKS)
    inner(sx)
    x_arrive()
    fill_sides(sx, xw)
    outer(sx)

    def store_y(i, value):
        yw[:, pl.ds(reach + i * width, width)] = value

    summed_rows(prods, codes, row_tiles, store_y)
    y_start()

    fill_own(sp, pw)
    inner(sp)
    p_arrive()
    fill_sides(sp, pw)
    outer(sp)

    def store_q(i, value):
        q[:, pl.ds(i * width, width)] = value

    summed_rows(prods, codes, row_tiles, store_q)

    pl.semaphore_wait(middle, 2)
    greet(far, {"rows": layer_by(2 * near)})
    greet(far, {"rows": layer_by(-2 * near)})

    fill_own(sy, yw)
    inner(sy)

    def gram_of(right):
        left = jnp.concatenate([xw[:, own], yw[:, own], pw[:, own]], axis=0)
        return lax.dot_general(
            left, right, (((1,), (1,)), ((), ())), precision=lax.Precision.HIGHEST,
            preferred_element_type=F32,
        )

    gram = gram_of(
        jnp.concatenate(
            [xw[:, own], yw[:, own], pw[:, own], q[...], jnp.zeros((4 * channels, here), F32)],
            axis=0,
        )
    )
    y_arrive()
    fill_sides(sy, yw)
    outer(sy)

    def store_z(i, value):
        z[:, pl.ds(i * width, width)] = value

    summed_rows(prods, codes, row_tiles, store_z)
    gram = gram + gram_of(
        jnp.concatenate(
            [jnp.zeros((4 * channels, here), F32), z[...], jnp.zeros((3 * channels, here), F32)],
            axis=0,
        )
    )
    gram_x, gram_y, gram_p = (gram[i * channels : (i + 1) * channels] for i in range(3))
    lane = lax.broadcasted_iota(jnp.int32, (channels, 128), 1)
    first = jnp.where(lane < 5 * channels, gram_x, pltpu.roll(gram_p, 3 * channels, 1))
    half = channels // 2
    lane = lax.broadcasted_iota(jnp.int32, (half, 128), 1)
    second = jnp.where(
        jnp.logical_and(lane >= channels, lane < 5 * channels),
        gram_y[:half], pltpu.roll(gram_y[half:], 64, 1),
    )
    packed = jnp.concatenate([first, second], axis=0)
    rows_each = PACKED // members
    for i in range(members):
        parts[i] = packed[i * rows_each : (i + 1) * rows_each]

    def spread(offset, incoming=False):
        other, device = member_by(offset)
        slot = other if incoming else member
        return pltpu.make_async_remote_copy(
            src_ref=parts.at[other], dst_ref=arrived.at[slot], send_sem=send_a.at[other],
            recv_sem=recv_a.at[slot], device_id=device, device_id_type=MESH,
        )

    def over(k, incoming=False):
        other = layer_at(k)
        slot = other if incoming else layer
        return pltpu.make_async_remote_copy(
            src_ref=along.at[layer], dst_ref=along.at[slot], send_sem=send_b.at[other],
            recv_sem=recv_b.at[slot], device_id={"rows": other}, device_id_type=MESH,
        )

    def share(offset, incoming=False):
        other, device = member_by(offset)
        slot = other if incoming else member
        return pltpu.make_async_remote_copy(
            src_ref=gathered.at[member], dst_ref=gathered.at[slot], send_sem=send_c.at[other],
            recv_sem=recv_c.at[slot], device_id=device, device_id_type=MESH,
        )

    others = range(1, members)
    for i in others:
        spread(i).start()
    arrived[member] = parts[member]
    outs = [
        pltpu.make_async_copy(yw.at[:, own], y_any, out_sems.at[0]),
        pltpu.make_async_copy(z, z_any, out_sems.at[1]),
    ]
    for out in outs:
        out.start()
    pl.semaphore_wait(far, 2)
    for i in others:
        spread(i, True).wait_recv()
    along[layer] = jnp.sum(arrived[...], axis=0)
    each(depth - 1, lambda k: over(k).start())
    x_finish()
    p_finish()
    y_finish()
    for out in outs:
        out.wait()
    for i in others:
        spread(i).wait_send()
    each(depth - 1, lambda k: over(k, True).wait_recv())
    gathered[member] = jnp.sum(along[...], axis=0)
    for i in others:
        share(i).start()
    each(depth - 1, lambda k: over(k).wait_send())
    for i in others:
        share(i, True).wait_recv()
    total_ref[...] = gathered[...]
    for i in others:
        share(i).wait_send()


def eliminated(matrix):
    n, lanes = matrix.shape
    block = 16
    pieces = [matrix[i : i + block] for i in range(0, n, block)]
    done = []
    for b in range(n // block):
        rest = jnp.concatenate(pieces[b:], axis=0) if b < n // block - 1 else pieces[b]
        tall = rest.shape[0]
        row = lax.broadcasted_iota(jnp.int32, (tall, lanes), 0)
        columns = [
            jnp.broadcast_to(rest[:, b * block + j : b * block + j + 1], (tall, lanes))
            for j in range(block)
        ]
        pivots = jnp.ones((block, lanes), F32)
        for j in range(block):
            pivot = columns[j][j : j + 1]
            inverse = 1.0 / pivot
            pivots = jnp.where(row[:block] == j, pivot, pivots)
            below = jnp.where(row > j, columns[j], 0.0)
            rest = rest - below * (rest[j : j + 1] * inverse)
            for i in range(j + 1, block):
                columns[i] = columns[i] - below * (columns[i][j : j + 1] * inverse)
        pieces[b:] = [rest[i : i + block] for i in range(0, tall, block)]
        done.append(pieces[b] * lax.rsqrt(pivots))
    return jnp.concatenate(done, axis=0) if len(done) > 1 else done[0]


def precise(left, right, turned=False):
    return lax.dot_general(
        left, right, (((1,), (1 if turned else 0,)), ((), ())),
        precision=lax.Precision.HIGHEST, preferred_element_type=F32,
    )


def dense_kernel(
    vertex_total, total_ref, x_any, y_any, z_any, locked_any, w_any, image_any, ritz,
    xs, ys, zs, w, image, locked_s, sems,
):
    channels = xs.shape[0]
    loads = [
        pltpu.make_async_copy(source, target, sems.at[i])
        for i, (source, target) in enumerate(
            ((locked_any, locked_s), (x_any, xs), (y_any, ys), (z_any, zs))
        )
    ]
    for load in loads:
        load.start()
    packed = jnp.concatenate([total_ref[i] for i in range(total_ref.shape[0])], axis=0)
    first, folded = packed[:channels], packed[channels:]

    def part(v, i):
        return v[:, i * channels : (i + 1) * channels]

    xx, xy, xp, xq, xz, pp, pq, pz = (part(first, i) for i in range(8))
    second = jnp.concatenate([folded, pltpu.roll(folded, 64, 1)], axis=0)
    yy, yp = part(second, 1), part(second, 2)
    shape = (channels, channels)
    row = lax.broadcasted_iota(jnp.int32, shape, 0)
    column = lax.broadcasted_iota(jnp.int32, shape, 1)
    eye = jnp.where(row == column, 1.0, 0.0).astype(F32)
    yx = xy.T
    top = eye * (xy + 1e-06)
    below = eye * (xx + 1e-06)
    c_down = jnp.sum(top, axis=1, keepdims=True) / jnp.sum(below, axis=1, keepdims=True)
    c_along = jnp.sum(top, axis=0, keepdims=True) / jnp.sum(below, axis=0, keepdims=True)
    loads[0].wait()
    locked = locked_s[0]
    free_down = (lax.broadcasted_iota(jnp.int32, (channels, 1), 0) >= locked).astype(F32)
    free_along = (lax.broadcasted_iota(jnp.int32, (1, channels), 1) >= locked).astype(F32)
    scale = 1.0 / vertex_total
    frozen = eye * (1.0 - free_down)
    rx = free_down * (c_down * xx - yx)
    ry = free_down * (c_down * xy - yy)
    gram_w = free_along * (rx * c_along - ry) * scale + frozen
    inverse = eliminated(jnp.concatenate([gram_w, eye], axis=1))[:, channels:]

    lane = lax.broadcasted_iota(jnp.int32, first.shape, 1)
    rd = jnp.where(lane < channels, jnp.concatenate([rx] * 8, axis=1), free_down * (c_down * first - second))
    wd = precise(inverse, rd)
    wx, wy, wp, wq, wz = (part(wd, i) for i in range(5))
    px, py = xp.T, yp.T

    def against_r(vx, vy):
        return free_along * (vx * c_along - vy)

    def against_image(vx, vy, vz):
        return free_along * (c_along * (vx - vy) - vy + vz)

    stacked = jnp.concatenate(
        [against_r(wx, wy), against_image(xx, xy, xz), against_image(wx, wy, wz),
         against_image(px, py, pz)], axis=0,
    )
    stacked = precise(stacked, inverse, turned=True)
    ww, xaw, waw, paw = (stacked[i * channels : (i + 1) * channels] for i in range(4))

    for load in loads[1:]:
        load.wait()
    r = free_down * (c_down * xs[...] - ys[...])
    nr = free_down * (c_down * ys[...] - zs[...])
    w[...] = precise(inverse, r)
    image[...] = precise(inverse, r - nr)
    stores = [
        pltpu.make_async_copy(w, w_any, sems.at[4]),
        pltpu.make_async_copy(image, image_any, sems.at[5]),
    ]
    for store in stores:
        store.start()

    gram_b = jnp.concatenate(
        [
            jnp.concatenate([xx, wx.T, xp], axis=1) * scale,
            jnp.concatenate([wx * scale, ww * scale + frozen, wp * scale], axis=1),
            jnp.concatenate([px, wp.T, pp], axis=1) * scale,
        ], axis=0,
    )
    gram_a = jnp.concatenate(
        [
            jnp.concatenate([xx - xy, xaw, xp - xq], axis=1),
            jnp.concatenate([wx - wy, waw, wp - wq], axis=1),
            jnp.concatenate([px - py, paw, pp - pq], axis=1),
        ], axis=0,
    ) * scale
    n = 3 * channels
    big = (
        lax.broadcasted_iota(jnp.int32, (n, n), 0) == lax.broadcasted_iota(jnp.int32, (n, n), 1)
    ).astype(F32)
    lower = eliminated(jnp.concatenate([gram_b, big], axis=1))[:, n:]
    symmetric = 0.5 * (gram_a + gram_a.T)
    ritz[...] = precise(precise(lower, symmetric), lower, turned=True)
    for store in stores:
        store.wait()


def body(sizes, current_block, previous_block, adjacency_tiles, tile_rows, tile_cols, tile_count, locked):
    channels, here = current_block.shape
    slots, width, _ = adjacency_tiles.shape
    depth, cols, sub = sizes
    members = cols * sub
    rows_each = PACKED // members
    span = 2 * here // width
    vmem = pl.BlockSpec(memory_space=pltpu.VMEM)
    anywhere = pl.BlockSpec(memory_space=pl.ANY)
    dma = pltpu.SemaphoreType.DMA
    regular = pltpu.SemaphoreType.REGULAR
    i32 = jnp.int32

    def like(*shape):
        return jax.ShapeDtypeStruct(shape, F32)

    total, y, z = pl.pallas_call(
        functools.partial(main_kernel, sizes),
        name="main",
        out_shape=(like(members, rows_each, 128), like(channels, here), like(channels, here)),
        in_specs=[anywhere] * 6,
        out_specs=(vmem, anywhere, anywhere),
        scratch_shapes=[
            VMEM((channels, 2 * here), F32),
            VMEM((channels, 2 * here), F32),
            VMEM((channels, 2 * here), F32),
            VMEM((span, 2 * channels, width), BF16),
            VMEM((span, 2 * channels, width), BF16),
            VMEM((span, 2 * channels, width), BF16),
            VMEM((slots, width, width), F32),
            VMEM((slots, width, 2 * width), BF16),
            VMEM((slots, channels, width), F32),
            VMEM((channels, here), F32),
            VMEM((channels, here), F32),
            VMEM((members, rows_each, 128), F32),
            VMEM((members, rows_each, 128), F32),
            VMEM((depth, rows_each, 128), F32),
            VMEM((members, rows_each, 128), F32),
            pltpu.SMEM((slots,), i32), pltpu.SMEM((slots,), i32),
            pltpu.SMEM((1,), i32), pltpu.SMEM((slots,), i32),
            dma((5,)), dma((CHUNKS,)), dma((6,)), dma((6,)),
            dma((members,)), dma((members,)),
            dma((depth,)), dma((depth,)),
            dma((members,)), dma((members,)),
            dma((2,)), regular, regular,
        ],
        compiler_params=pltpu.CompilerParams(collective_id=0, has_side_effects=True),
    )(current_block, previous_block, adjacency_tiles, tile_rows, tile_cols, tile_count)
    return pl.pallas_call(
        functools.partial(dense_kernel, float(here * depth * members)),
        name="dense",
        out_shape=(like(channels, here), like(channels, here), like(3 * channels, 3 * channels)),
        in_specs=[vmem] + [anywhere] * 4,
        out_specs=(anywhere, anywhere, vmem),
        scratch_shapes=[VMEM((channels, here), F32)] * 5
        + [pltpu.SMEM((1,), i32), dma((6,))],
    )(total, current_block, y, z, locked)


def solution(mesh):
    sizes = tuple(mesh.shape[a] for a in VERTEX_AXES)
    everywhere = ("graphs", "rows", "cols", "sub")
    in_specs = (
        P(None, everywhere),
        P(None, everywhere),
        P(everywhere, None, None),
        P(everywhere),
        P(everywhere),
        P(everywhere),
        P("graphs"),
    )
    out_specs = (P(None, everywhere), P(None, everywhere), P("graphs", None))
    return jax.shard_map(
        functools.partial(body, sizes), mesh=mesh, in_specs=in_specs, out_specs=out_specs,
        check_vma=False,
    )
```

```python
import functools

import jax
import jax.numpy as jnp
from jax import lax
from jax.experimental import pallas as pl
from jax.experimental.pallas import tpu as pltpu
from jax.sharding import PartitionSpec as P

MESH = pl.DeviceIdType.MESH
F32 = jnp.float32
BF16 = jnp.bfloat16
VMEM = pltpu.VMEM
VERTEX_AXES = ("rows", "cols", "sub")
CHUNKS = 4
GROUP = 8
PACKED = 24


def halves(value):
    high = value.astype(BF16)
    return high, (value - high.astype(F32)).astype(BF16)


def tile_copies(tiles_ref, tiles, sems):
    each = tiles.shape[0] // CHUNKS
    return [
        pltpu.make_async_copy(
            tiles_ref.at[pl.ds(i * each, each)], tiles.at[pl.ds(i * each, each)], sems.at[i]
        )
        for i in range(CHUNKS)
    ]


def fill_tiles(split, first, value):
    width = split.shape[2]
    for i in range(value.shape[1] // width):
        split[first + i] = jnp.concatenate(halves(value[:, i * width : (i + 1) * width]), axis=0)


def split_tiles(tiles, pairs, first, last):
    def step(block, carry):
        for lane in range(GROUP // 2):
            slot = block * (GROUP // 2) + lane
            pairs[slot] = jnp.concatenate(halves(tiles[slot]), axis=1)
        return carry

    lax.fori_loop(first // (GROUP // 2), last // (GROUP // 2), step, 0)


def products(split, pairs, prods, first, last, column):
    width = pairs.shape[1]
    channels = split.shape[1] // 2

    def step(block, carry):
        for lane in range(GROUP):
            slot = block * GROUP + lane
            out = jnp.dot(split[column(slot)], pairs[slot], preferred_element_type=F32)
            top, bottom = out[:channels], out[channels:]
            prods[slot] = (
                top[:, :width] + (top[:, width:] + bottom[:, :width])
            ) + bottom[:, width:]
        return carry

    lax.fori_loop(first // GROUP, last // GROUP, step, 0)


def summed_rows(prods, codes, row_tiles, store):
    slots, channels, width = prods.shape
    size = row_tiles // 2
    for block in range(2):
        mine = [block * size + i for i in range(size)]

        def step(slot, sums):
            value = prods[slot]
            row = jnp.full((channels, width), codes[slot], jnp.int32)
            return tuple(s + jnp.where(row == i, value, 0.0) for i, s in zip(mine, sums))

        sums = lax.fori_loop(
            row_tiles, slots, step, tuple(prods[i] for i in mine), unroll=4
        )
        for i, s in zip(mine, sums):
            store(i, s)


def place(sizes):
    rows, cols, sub = (lax.axis_index(a) for a in VERTEX_AXES)
    return (rows * sizes[1] + cols) * sizes[2] + sub


def device_at(position, sizes):
    return {
        "rows": lax.div(position, sizes[1] * sizes[2]),
        "cols": lax.rem(lax.div(position, sizes[2]), sizes[1]),
        "sub": lax.rem(position, sizes[2]),
    }


def main_kernel(
    sizes, x_any, p_any, tiles_any, rows_any, cols_any, count_any, total_ref, y_any, z_any,
    xw, pw, yw, sx, sp, sy, tiles, pairs, prods, q, z, parts, arrived, along, gathered,
    rows_s, cols_s, count_s, codes, load_sems, tile_sems, halo_send, halo_recv,
    send_a, recv_a, send_b, recv_b, send_c, recv_c, out_sems, from_low, from_high, gram_s,
):
    channels, here = q.shape
    slots, width, _ = tiles.shape
    row_tiles = here // width
    reach = here // 2
    reach_tiles = reach // width
    depth, cols, sub = sizes
    members = cols * sub
    total = depth * members
    me = place(sizes)
    base = me * row_tiles
    layer = lax.axis_index("rows")
    member = lax.axis_index("cols") * sub + lax.axis_index("sub")
    near = max(1, depth // 16)
    stages = [near]
    while 2 * stages[-1] < depth // 2:
        stages.append(2 * stages[-1])
    own = pl.ds(reach, here)
    low_side, high_side = pl.ds(0, reach), pl.ds(reach + here, reach)

    def layer_by(offset):
        other = layer + offset
        other = jnp.where(other >= depth, other - depth, other)
        return jnp.where(other < 0, other + depth, other)

    def layer_at(k):
        return layer_by(k + 1)

    def member_by(offset):
        other = member + offset
        other = jnp.where(other >= members, other - members, other)
        return other, {"cols": lax.div(other, sub), "sub": lax.rem(other, sub)}

    def each(n, act):
        def step(k, carry):
            act(k)
            return carry

        lax.fori_loop(0, n, step, 0)

    def tell(stage):
        greet(from_low.at[stage], {"rows": layer_by(stages[stage])})
        greet(from_high.at[stage], {"rows": layer_by(-stages[stage])})

    def hear(stage):
        pl.semaphore_wait(from_low.at[stage], 1)
        pl.semaphore_wait(from_high.at[stage], 1)

    last = len(stages) - 1
    barrier = pltpu.get_barrier_semaphore()

    def greet(semaphore, device):
        pl.semaphore_signal(semaphore, inc=1, device_id=device, device_id_type=MESH)

    has_low, has_high = me > 0, me < total - 1
    low = device_at(jnp.maximum(me - 1, 0), sizes)
    high = device_at(jnp.minimum(me + 1, total - 1), sizes)

    load_x = pltpu.make_async_copy(x_any, xw.at[:, own], load_sems.at[0])
    load_x.start()

    @pl.when(has_low)
    def _():
        greet(barrier, low)

    @pl.when(has_high)
    def _():
        greet(barrier, high)

    for offset in range(1, members):
        greet(barrier, member_by(offset)[1])
    for offset in range(1, near + 1):
        greet(barrier, {"rows": layer_by(offset)})
        greet(barrier, {"rows": layer_by(-offset)})
    load_p = pltpu.make_async_copy(p_any, pw.at[:, own], load_sems.at[1])
    small = [
        pltpu.make_async_copy(source, target, load_sems.at[2 + i])
        for i, (source, target) in enumerate(
            ((rows_any, rows_s), (cols_any, cols_s), (count_any, count_s))
        )
    ]
    loads = tile_copies(tiles_any, tiles, tile_sems)
    for load in [load_p, *small, *loads]:
        load.start()
    pl.semaphore_wait(
        barrier,
        has_low.astype(jnp.int32) + has_high.astype(jnp.int32) + (members - 1 + 2 * near),
    )

    def halo(wide, n):
        def remote(source, target, k, device):
            return pltpu.make_async_remote_copy(
                src_ref=wide.at[:, source], dst_ref=wide.at[:, target],
                send_sem=halo_send.at[k], recv_sem=halo_recv.at[k],
                device_id=device, device_id_type=MESH,
            )

        down = remote(pl.ds(reach, reach), high_side, 2 * n, low)
        up = remote(pl.ds(here, reach), low_side, 2 * n + 1, high)

        def start():
            @pl.when(has_low)
            def _():
                down.start()

            @pl.when(has_high)
            def _():
                up.start()

        def arrive():
            @pl.when(has_low)
            def _():
                up.wait_recv()

            @pl.when(has_high)
            def _():
                down.wait_recv()

        def finish():
            @pl.when(has_low)
            def _():
                down.wait_send()

            @pl.when(has_high)
            def _():
                up.wait_send()

        return start, arrive, finish

    x_start, x_arrive, x_finish = halo(xw, 0)
    p_start, p_arrive, p_finish = halo(pw, 1)
    y_start, y_arrive, y_finish = halo(yw, 2)

    load_x.wait()
    x_start()
    load_p.wait()
    p_start()
    tell(0)

    @pl.when(jnp.logical_not(has_low))
    def _():
        for wide in (xw, pw, yw):
            wide[:, low_side] = jnp.zeros((channels, reach), F32)

    @pl.when(jnp.logical_not(has_high))
    def _():
        for wide in (xw, pw, yw):
            wide[:, high_side] = jnp.zeros((channels, reach), F32)

    for load in small:
        load.wait()
    count = count_s[0]

    def code(slot):
        codes[slot] = jnp.where(slot < count, rows_s[slot] - base, -1)

    each(slots, code)

    def column(slot):
        return jnp.clip(cols_s[slot] - (base - reach_tiles), 0, 2 * row_tiles - 1)

    def inner(split):
        products(split, pairs, prods, 0, row_tiles, lambda slot: slot + reach_tiles)

    def outer(split):
        products(split, pairs, prods, row_tiles, slots, column)

    def fill_own(split, wide):
        fill_tiles(split, reach_tiles, wide[:, own])

    def fill_sides(split, wide):
        fill_tiles(split, 0, wide[:, low_side])
        fill_tiles(split, reach_tiles + row_tiles, wide[:, high_side])

    fill_own(sx, xw)
    for i, load in enumerate(loads):
        load.wait()
        split_tiles(tiles, pairs, i * slots // CHUNKS, (i + 1) * slots // CHUNKS)
    inner(sx)
    for stage in range(last - 1):
        hear(stage)
        tell(stage + 1)
    x_arrive()
    fill_sides(sx, xw)
    outer(sx)

    def store_y(i, value):
        yw[:, pl.ds(reach + i * width, width)] = value

    summed_rows(prods, codes, row_tiles, store_y)
    y_start()

    fill_own(sp, pw)
    inner(sp)
    p_arrive()
    fill_sides(sp, pw)
    outer(sp)

    def store_q(i, value):
        q[:, pl.ds(i * width, width)] = value

    summed_rows(prods, codes, row_tiles, store_q)

    hear(last - 1)
    tell(last)

    fill_own(sy, yw)
    inner(sy)

    def gram_of(right):
        left = jnp.concatenate([xw[:, own], yw[:, own], pw[:, own]], axis=0)
        return lax.dot_general(
            left, right, (((1,), (1,)), ((), ())), precision=lax.Precision.HIGHEST,
            preferred_element_type=F32,
        )

    gram_s[...] = gram_of(
        jnp.concatenate(
            [xw[:, own], yw[:, own], pw[:, own], q[...], jnp.zeros((4 * channels, here), F32)],
            axis=0,
        )
    )
    y_arrive()
    fill_sides(sy, yw)
    outer(sy)

    def store_z(i, value):
        z[:, pl.ds(i * width, width)] = value

    summed_rows(prods, codes, row_tiles, store_z)
    with_z = gram_of(z[...])
    with_z = jnp.concatenate([with_z, jnp.zeros((3 * channels, 128 - channels), F32)], axis=1)
    gram = gram_s[...] + pltpu.roll(with_z, 4 * channels, 1)
    gram_x, gram_y, gram_p = (gram[i * channels : (i + 1) * channels] for i in range(3))
    lane = lax.broadcasted_iota(jnp.int32, (channels, 128), 1)
    first = jnp.where(lane < 5 * channels, gram_x, pltpu.roll(gram_p, 3 * channels, 1))
    half = channels // 2
    lane = lax.broadcasted_iota(jnp.int32, (half, 128), 1)
    second = jnp.where(
        jnp.logical_and(lane >= channels, lane < 5 * channels),
        gram_y[:half], pltpu.roll(gram_y[half:], 64, 1),
    )
    packed = jnp.concatenate([first, second], axis=0)
    rows_each = PACKED // members
    for i in range(members):
        parts[i] = packed[i * rows_each : (i + 1) * rows_each]

    def spread(offset, incoming=False):
        other, device = member_by(offset)
        slot = other if incoming else member
        return pltpu.make_async_remote_copy(
            src_ref=parts.at[other], dst_ref=arrived.at[slot], send_sem=send_a.at[other],
            recv_sem=recv_a.at[slot], device_id=device, device_id_type=MESH,
        )

    def over(k, incoming=False):
        other = layer_at(k)
        slot = other if incoming else layer
        return pltpu.make_async_remote_copy(
            src_ref=along.at[layer], dst_ref=along.at[slot], send_sem=send_b.at[other],
            recv_sem=recv_b.at[slot], device_id={"rows": other}, device_id_type=MESH,
        )

    def share(offset, incoming=False):
        other, device = member_by(offset)
        slot = other if incoming else member
        return pltpu.make_async_remote_copy(
            src_ref=gathered.at[member], dst_ref=gathered.at[slot], send_sem=send_c.at[other],
            recv_sem=recv_c.at[slot], device_id=device, device_id_type=MESH,
        )

    others = range(1, members)
    for i in others:
        spread(i).start()
    arrived[member] = parts[member]
    outs = [
        pltpu.make_async_copy(yw.at[:, own], y_any, out_sems.at[0]),
        pltpu.make_async_copy(z, z_any, out_sems.at[1]),
    ]
    for out in outs:
        out.start()
    for i in others:
        spread(i, True).wait_recv()
    along[layer] = jnp.sum(arrived[...], axis=0)
    pl.semaphore_wait(from_low.at[last], 1)
    for k in range(depth // 2, depth - stages[last]):
        over(k - 1).start()
    pl.semaphore_wait(from_high.at[last], 1)
    for k in range(depth // 2 - 1, 0, -1):
        over(k - 1).start()
        if k < stages[last]:
            over(depth - k - 1).start()
    over(depth - stages[last] - 1).start()
    x_finish()
    p_finish()
    y_finish()
    for out in outs:
        out.wait()
    for i in others:
        spread(i).wait_send()
    each(depth - 1, lambda k: over(k, True).wait_recv())
    gathered[member] = jnp.sum(along[...], axis=0)
    for i in others:
        share(i).start()
    each(depth - 1, lambda k: over(k).wait_send())
    for i in others:
        share(i, True).wait_recv()
    total_ref[...] = gathered[...]
    for i in others:
        share(i).wait_send()


def eliminated(matrix):
    n, lanes = matrix.shape
    block = 16
    pieces = [matrix[i : i + block] for i in range(0, n, block)]
    done = []
    for b in range(n // block):
        rest = jnp.concatenate(pieces[b:], axis=0) if b < n // block - 1 else pieces[b]
        tall = rest.shape[0]
        row = lax.broadcasted_iota(jnp.int32, (tall, lanes), 0)
        columns = [
            jnp.broadcast_to(rest[:, b * block + j : b * block + j + 1], (tall, lanes))
            for j in range(block)
        ]
        pivots = jnp.ones((block, lanes), F32)
        for j in range(block):
            pivot = columns[j][j : j + 1]
            inverse = 1.0 / pivot
            pivots = jnp.where(row[:block] == j, pivot, pivots)
            below = jnp.where(row > j, columns[j], 0.0)
            rest = rest - below * (rest[j : j + 1] * inverse)
            for i in range(j + 1, block):
                columns[i] = columns[i] - below * (columns[i][j : j + 1] * inverse)
        pieces[b:] = [rest[i : i + block] for i in range(0, tall, block)]
        done.append(pieces[b] * lax.rsqrt(pivots))
    return jnp.concatenate(done, axis=0) if len(done) > 1 else done[0]


def precise(left, right, turned=False):
    return lax.dot_general(
        left, right, (((1,), (1 if turned else 0,)), ((), ())),
        precision=lax.Precision.HIGHEST, preferred_element_type=F32,
    )


def dense_kernel(
    vertex_total, total_ref, x_any, y_any, z_any, locked_any, w_any, image_any, ritz,
    xs, ys, zs, w, image, locked_s, sems,
):
    channels = xs.shape[0]
    loads = [
        pltpu.make_async_copy(source, target, sems.at[i])
        for i, (source, target) in enumerate(
            ((locked_any, locked_s), (x_any, xs), (y_any, ys), (z_any, zs))
        )
    ]
    for load in loads:
        load.start()
    packed = jnp.concatenate([total_ref[i] for i in range(total_ref.shape[0])], axis=0)
    first, folded = packed[:channels], packed[channels:]

    def part(v, i):
        return v[:, i * channels : (i + 1) * channels]

    xx, xy, xp, xq, xz, pp, pq, pz = (part(first, i) for i in range(8))
    second = jnp.concatenate([folded, pltpu.roll(folded, 64, 1)], axis=0)
    yy, yp = part(second, 1), part(second, 2)
    shape = (channels, channels)
    row = lax.broadcasted_iota(jnp.int32, shape, 0)
    column = lax.broadcasted_iota(jnp.int32, shape, 1)
    eye = jnp.where(row == column, 1.0, 0.0).astype(F32)
    yx = xy.T
    top = eye * (xy + 1e-06)
    below = eye * (xx + 1e-06)
    c_down = jnp.sum(top, axis=1, keepdims=True) / jnp.sum(below, axis=1, keepdims=True)
    c_along = jnp.sum(top, axis=0, keepdims=True) / jnp.sum(below, axis=0, keepdims=True)
    loads[0].wait()
    locked = locked_s[0]
    free_down = (lax.broadcasted_iota(jnp.int32, (channels, 1), 0) >= locked).astype(F32)
    free_along = (lax.broadcasted_iota(jnp.int32, (1, channels), 1) >= locked).astype(F32)
    scale = 1.0 / vertex_total
    frozen = eye * (1.0 - free_down)
    rx = free_down * (c_down * xx - yx)
    ry = free_down * (c_down * xy - yy)
    gram_w = free_along * (rx * c_along - ry) * scale + frozen
    inverse = eliminated(jnp.concatenate([gram_w, eye], axis=1))[:, channels:]

    lane = lax.broadcasted_iota(jnp.int32, first.shape, 1)
    rd = jnp.where(lane < channels, jnp.concatenate([rx] * 8, axis=1), free_down * (c_down * first - second))
    wd = precise(inverse, rd)
    wx, wy, wp, wq, wz = (part(wd, i) for i in range(5))
    px, py = xp.T, yp.T

    def against_r(vx, vy):
        return free_along * (vx * c_along - vy)

    def against_image(vx, vy, vz):
        return free_along * (c_along * (vx - vy) - vy + vz)

    stacked = jnp.concatenate(
        [against_r(wx, wy), against_image(xx, xy, xz), against_image(wx, wy, wz),
         against_image(px, py, pz)], axis=0,
    )
    stacked = precise(stacked, inverse, turned=True)
    ww, xaw, waw, paw = (stacked[i * channels : (i + 1) * channels] for i in range(4))

    for load in loads[1:]:
        load.wait()
    r = free_down * (c_down * xs[...] - ys[...])
    nr = free_down * (c_down * ys[...] - zs[...])
    w[...] = precise(inverse, r)
    image[...] = precise(inverse, r - nr)
    stores = [
        pltpu.make_async_copy(w, w_any, sems.at[4]),
        pltpu.make_async_copy(image, image_any, sems.at[5]),
    ]
    for store in stores:
        store.start()

    gram_b = jnp.concatenate(
        [
            jnp.concatenate([xx, wx.T, xp], axis=1) * scale,
            jnp.concatenate([wx * scale, ww * scale + frozen, wp * scale], axis=1),
            jnp.concatenate([px, wp.T, pp], axis=1) * scale,
        ], axis=0,
    )
    gram_a = jnp.concatenate(
        [
            jnp.concatenate([xx - xy, xaw, xp - xq], axis=1),
            jnp.concatenate([wx - wy, waw, wp - wq], axis=1),
            jnp.concatenate([px - py, paw, pp - pq], axis=1),
        ], axis=0,
    ) * scale
    n = 3 * channels
    big = (
        lax.broadcasted_iota(jnp.int32, (n, n), 0) == lax.broadcasted_iota(jnp.int32, (n, n), 1)
    ).astype(F32)
    lower = eliminated(jnp.concatenate([gram_b, big], axis=1))[:, n:]
    symmetric = 0.5 * (gram_a + gram_a.T)
    ritz[...] = precise(precise(lower, symmetric), lower, turned=True)
    for store in stores:
        store.wait()


def body(sizes, current_block, previous_block, adjacency_tiles, tile_rows, tile_cols, tile_count, locked):
    channels, here = current_block.shape
    slots, width, _ = adjacency_tiles.shape
    depth, cols, sub = sizes
    members = cols * sub
    rows_each = PACKED // members
    span = 2 * here // width
    vmem = pl.BlockSpec(memory_space=pltpu.VMEM)
    anywhere = pl.BlockSpec(memory_space=pltpu.HBM)
    dma = pltpu.SemaphoreType.DMA
    regular = pltpu.SemaphoreType.REGULAR
    i32 = jnp.int32

    def like(*shape):
        return jax.ShapeDtypeStruct(shape, F32)

    total, y, z = pl.pallas_call(
        functools.partial(main_kernel, sizes),
        name="main",
        out_shape=(like(members, rows_each, 128), like(channels, here), like(channels, here)),
        in_specs=[anywhere] * 6,
        out_specs=(vmem, anywhere, anywhere),
        scratch_shapes=[
            VMEM((channels, 2 * here), F32),
            VMEM((channels, 2 * here), F32),
            VMEM((channels, 2 * here), F32),
            VMEM((span, 2 * channels, width), BF16),
            VMEM((span, 2 * channels, width), BF16),
            VMEM((span, 2 * channels, width), BF16),
            VMEM((slots, width, width), F32),
            VMEM((slots, width, 2 * width), BF16),
            VMEM((slots, channels, width), F32),
            VMEM((channels, here), F32),
            VMEM((channels, here), F32),
            VMEM((members, rows_each, 128), F32),
            VMEM((members, rows_each, 128), F32),
            VMEM((depth, rows_each, 128), F32),
            VMEM((members, rows_each, 128), F32),
            pltpu.SMEM((slots,), i32), pltpu.SMEM((slots,), i32),
            pltpu.SMEM((1,), i32), pltpu.SMEM((slots,), i32),
            dma((5,)), dma((CHUNKS,)), dma((6,)), dma((6,)),
            dma((members,)), dma((members,)),
            dma((depth,)), dma((depth,)),
            dma((members,)), dma((members,)),
            dma((2,)), regular((4,)), regular((4,)), VMEM((3 * channels, 128), F32),
        ],
        compiler_params=pltpu.CompilerParams(collective_id=0, has_side_effects=True),
    )(current_block, previous_block, adjacency_tiles, tile_rows, tile_cols, tile_count)
    return pl.pallas_call(
        functools.partial(dense_kernel, float(here * depth * members)),
        name="dense",
        out_shape=(like(channels, here), like(channels, here), like(3 * channels, 3 * channels)),
        in_specs=[vmem] + [anywhere] * 4,
        out_specs=(anywhere, anywhere, vmem),
        scratch_shapes=[VMEM((channels, here), F32)] * 5
        + [pltpu.SMEM((1,), i32), dma((6,))],
    )(total, current_block, y, z, locked)


def solution(mesh):
    sizes = tuple(mesh.shape[a] for a in VERTEX_AXES)
    everywhere = ("graphs", "rows", "cols", "sub")
    in_specs = (
        P(None, everywhere),
        P(None, everywhere),
        P(everywhere, None, None),
        P(everywhere),
        P(everywhere),
        P(everywhere),
        P("graphs"),
    )
    out_specs = (P(None, everywhere), P(None, everywhere), P("graphs", None))
    return jax.shard_map(
        functools.partial(body, sizes), mesh=mesh, in_specs=in_specs, out_specs=out_specs,
        check_vma=False,
    )
```

```python
import functools

import jax
import jax.numpy as jnp
from jax import lax
from jax.experimental import pallas as pl
from jax.experimental.pallas import tpu as pltpu
from jax.sharding import PartitionSpec as P

MESH = pl.DeviceIdType.MESH
F32 = jnp.float32
BF16 = jnp.bfloat16
VMEM = pltpu.VMEM
VERTEX_AXES = ("rows", "cols", "sub")
CHUNKS = 4
GROUP = 8
PACKED = 24


def halves(value):
    high = value.astype(BF16)
    return high, (value - high.astype(F32)).astype(BF16)


def tile_copies(tiles_ref, tiles, sems):
    each = tiles.shape[0] // CHUNKS
    return [
        pltpu.make_async_copy(
            tiles_ref.at[pl.ds(i * each, each)], tiles.at[pl.ds(i * each, each)], sems.at[i]
        )
        for i in range(CHUNKS)
    ]


def fill_tiles(split, first, value):
    width = split.shape[2]
    for i in range(value.shape[1] // width):
        split[first + i] = jnp.concatenate(halves(value[:, i * width : (i + 1) * width]), axis=0)


def split_tiles(tiles, pairs, first, last):
    def step(block, carry):
        for lane in range(GROUP // 2):
            slot = block * (GROUP // 2) + lane
            pairs[slot] = jnp.concatenate(halves(tiles[slot]), axis=1)
        return carry

    lax.fori_loop(first // (GROUP // 2), last // (GROUP // 2), step, 0)


def products(split, pairs, prods, first, last, column):
    width = pairs.shape[1]
    channels = split.shape[1] // 2

    def step(block, carry):
        for lane in range(GROUP):
            slot = block * GROUP + lane
            out = jnp.dot(split[column(slot)], pairs[slot], preferred_element_type=F32)
            top, bottom = out[:channels], out[channels:]
            prods[slot] = (
                top[:, :width] + (top[:, width:] + bottom[:, :width])
            ) + bottom[:, width:]
        return carry

    lax.fori_loop(first // GROUP, last // GROUP, step, 0)


def summed_rows(prods, codes, row_tiles, store, after=None):
    slots, channels, width = prods.shape
    size = row_tiles // 2
    for block in range(2):
        mine = [block * size + i for i in range(size)]

        def step(slot, sums):
            value = prods[slot]
            row = jnp.full((channels, width), codes[slot], jnp.int32)
            return tuple(s + jnp.where(row == i, value, 0.0) for i, s in zip(mine, sums))

        sums = lax.fori_loop(
            row_tiles, slots, step, tuple(prods[i] for i in mine), unroll=4
        )
        for i, s in zip(mine, sums):
            store(i, s)
        if after is not None:
            after[block]()


def place(sizes):
    rows, cols, sub = (lax.axis_index(a) for a in VERTEX_AXES)
    return (rows * sizes[1] + cols) * sizes[2] + sub


def device_at(position, sizes):
    return {
        "rows": lax.div(position, sizes[1] * sizes[2]),
        "cols": lax.rem(lax.div(position, sizes[2]), sizes[1]),
        "sub": lax.rem(position, sizes[2]),
    }


def main_kernel(
    sizes, x_any, p_any, tiles_any, rows_any, cols_any, count_any, total_ref, y_any, z_any,
    xw, pw, yw, sx, sp, sy, tiles, pairs, prods, q, z, parts, arrived, along, gathered,
    rows_s, cols_s, count_s, codes, load_sems, tile_sems, halo_send, halo_recv,
    send_a, recv_a, send_b, recv_b, send_c, recv_c, out_sems, from_low, from_high, gram_s,
):
    channels, here = q.shape
    slots, width, _ = tiles.shape
    row_tiles = here // width
    reach = here // 2
    reach_tiles = reach // width
    depth, cols, sub = sizes
    members = cols * sub
    total = depth * members
    me = place(sizes)
    base = me * row_tiles
    layer = lax.axis_index("rows")
    member = lax.axis_index("cols") * sub + lax.axis_index("sub")
    near = max(1, depth // 16)
    stages = [near]
    while 2 * stages[-1] < depth // 2:
        stages.append(2 * stages[-1])
    own = pl.ds(reach, here)
    low_side, high_side = pl.ds(0, reach), pl.ds(reach + here, reach)

    def layer_by(offset):
        other = layer + offset
        other = jnp.where(other >= depth, other - depth, other)
        return jnp.where(other < 0, other + depth, other)

    def layer_at(k):
        return layer_by(k + 1)

    def member_by(offset):
        other = member + offset
        other = jnp.where(other >= members, other - members, other)
        return other, {"cols": lax.div(other, sub), "sub": lax.rem(other, sub)}

    def each(n, act):
        def step(k, carry):
            act(k)
            return carry

        lax.fori_loop(0, n, step, 0)

    def tell(stage):
        greet(from_low.at[stage], {"rows": layer_by(stages[stage])})
        greet(from_high.at[stage], {"rows": layer_by(-stages[stage])})

    def hear(stage):
        pl.semaphore_wait(from_low.at[stage], 1)
        pl.semaphore_wait(from_high.at[stage], 1)

    last = len(stages) - 1
    barrier = pltpu.get_barrier_semaphore()

    def greet(semaphore, device):
        pl.semaphore_signal(semaphore, inc=1, device_id=device, device_id_type=MESH)

    has_low, has_high = me > 0, me < total - 1
    low = device_at(jnp.maximum(me - 1, 0), sizes)
    high = device_at(jnp.minimum(me + 1, total - 1), sizes)

    load_x = pltpu.make_async_copy(x_any, xw.at[:, own], load_sems.at[0])
    load_x.start()

    @pl.when(has_low)
    def _():
        greet(barrier, low)

    @pl.when(has_high)
    def _():
        greet(barrier, high)

    for offset in range(1, members):
        greet(barrier, member_by(offset)[1])
    for offset in range(1, near + 1):
        greet(barrier, {"rows": layer_by(offset)})
        greet(barrier, {"rows": layer_by(-offset)})
    load_p = pltpu.make_async_copy(p_any, pw.at[:, own], load_sems.at[1])
    small = [
        pltpu.make_async_copy(source, target, load_sems.at[2 + i])
        for i, (source, target) in enumerate(
            ((rows_any, rows_s), (cols_any, cols_s), (count_any, count_s))
        )
    ]
    loads = tile_copies(tiles_any, tiles, tile_sems)
    for load in [load_p, *small, *loads]:
        load.start()
    pl.semaphore_wait(
        barrier,
        has_low.astype(jnp.int32) + has_high.astype(jnp.int32) + (members - 1 + 2 * near),
    )

    def halo(wide, n):
        def remote(source, target, k, device):
            return pltpu.make_async_remote_copy(
                src_ref=wide.at[:, source], dst_ref=wide.at[:, target],
                send_sem=halo_send.at[k], recv_sem=halo_recv.at[k],
                device_id=device, device_id_type=MESH,
            )

        down = remote(pl.ds(reach, reach), high_side, 2 * n, low)
        up = remote(pl.ds(here, reach), low_side, 2 * n + 1, high)

        def start_down():
            @pl.when(has_low)
            def _():
                down.start()

        def start_up():
            @pl.when(has_high)
            def _():
                up.start()

        def arrive():
            @pl.when(has_low)
            def _():
                up.wait_recv()

            @pl.when(has_high)
            def _():
                down.wait_recv()

        def finish():
            @pl.when(has_low)
            def _():
                down.wait_send()

            @pl.when(has_high)
            def _():
                up.wait_send()

        return (start_down, start_up), arrive, finish

    x_start, x_arrive, x_finish = halo(xw, 0)
    p_start, p_arrive, p_finish = halo(pw, 1)
    y_start, y_arrive, y_finish = halo(yw, 2)

    load_x.wait()
    for start in x_start:
        start()
    load_p.wait()
    for start in p_start:
        start()
    tell(0)

    @pl.when(jnp.logical_not(has_low))
    def _():
        for wide in (xw, pw, yw):
            wide[:, low_side] = jnp.zeros((channels, reach), F32)

    @pl.when(jnp.logical_not(has_high))
    def _():
        for wide in (xw, pw, yw):
            wide[:, high_side] = jnp.zeros((channels, reach), F32)

    for load in small:
        load.wait()
    count = count_s[0]

    def code(slot):
        codes[slot] = jnp.where(slot < count, rows_s[slot] - base, -1)

    each(slots, code)

    def column(slot):
        return jnp.clip(cols_s[slot] - (base - reach_tiles), 0, 2 * row_tiles - 1)

    def inner(split):
        products(split, pairs, prods, 0, row_tiles, lambda slot: slot + reach_tiles)

    def outer(split):
        products(split, pairs, prods, row_tiles, slots, column)

    def fill_own(split, wide):
        fill_tiles(split, reach_tiles, wide[:, own])

    def fill_sides(split, wide):
        fill_tiles(split, 0, wide[:, low_side])
        fill_tiles(split, reach_tiles + row_tiles, wide[:, high_side])

    fill_own(sx, xw)
    for i, load in enumerate(loads):
        load.wait()
        split_tiles(tiles, pairs, i * slots // CHUNKS, (i + 1) * slots // CHUNKS)
    inner(sx)
    for stage in range(last - 1):
        hear(stage)
        tell(stage + 1)
    x_arrive()
    fill_sides(sx, xw)
    outer(sx)

    def store_y(i, value):
        yw[:, pl.ds(reach + i * width, width)] = value

    summed_rows(prods, codes, row_tiles, store_y, y_start)

    fill_own(sp, pw)
    inner(sp)
    p_arrive()
    fill_sides(sp, pw)
    outer(sp)

    def store_q(i, value):
        q[:, pl.ds(i * width, width)] = value

    summed_rows(prods, codes, row_tiles, store_q)

    hear(last - 1)
    tell(last)

    fill_own(sy, yw)
    inner(sy)

    def gram_of(right):
        left = jnp.concatenate([xw[:, own], yw[:, own], pw[:, own]], axis=0)
        return lax.dot_general(
            left, right, (((1,), (1,)), ((), ())), precision=lax.Precision.HIGHEST,
            preferred_element_type=F32,
        )

    gram_s[...] = gram_of(
        jnp.concatenate(
            [xw[:, own], yw[:, own], pw[:, own], q[...], jnp.zeros((4 * channels, here), F32)],
            axis=0,
        )
    )
    y_arrive()
    fill_sides(sy, yw)
    outer(sy)

    def store_z(i, value):
        z[:, pl.ds(i * width, width)] = value

    summed_rows(prods, codes, row_tiles, store_z)
    with_z = gram_of(z[...])
    with_z = jnp.concatenate([with_z, jnp.zeros((3 * channels, 128 - channels), F32)], axis=1)
    gram = gram_s[...] + pltpu.roll(with_z, 4 * channels, 1)
    gram_x, gram_y, gram_p = (gram[i * channels : (i + 1) * channels] for i in range(3))
    lane = lax.broadcasted_iota(jnp.int32, (channels, 128), 1)
    first = jnp.where(lane < 5 * channels, gram_x, pltpu.roll(gram_p, 3 * channels, 1))
    half = channels // 2
    lane = lax.broadcasted_iota(jnp.int32, (half, 128), 1)
    second = jnp.where(
        jnp.logical_and(lane >= channels, lane < 5 * channels),
        gram_y[:half], pltpu.roll(gram_y[half:], 64, 1),
    )
    packed = jnp.concatenate([first, second], axis=0)
    rows_each = PACKED // members
    for i in range(members):
        parts[i] = packed[i * rows_each : (i + 1) * rows_each]

    def spread(offset, incoming=False):
        other, device = member_by(offset)
        slot = other if incoming else member
        return pltpu.make_async_remote_copy(
            src_ref=parts.at[other], dst_ref=arrived.at[slot], send_sem=send_a.at[other],
            recv_sem=recv_a.at[slot], device_id=device, device_id_type=MESH,
        )

    def over(k, incoming=False):
        other = layer_at(k)
        slot = other if incoming else layer
        return pltpu.make_async_remote_copy(
            src_ref=along.at[layer], dst_ref=along.at[slot], send_sem=send_b.at[other],
            recv_sem=recv_b.at[slot], device_id={"rows": other}, device_id_type=MESH,
        )

    def share(offset, incoming=False):
        other, device = member_by(offset)
        slot = other if incoming else member
        return pltpu.make_async_remote_copy(
            src_ref=gathered.at[member], dst_ref=gathered.at[slot], send_sem=send_c.at[other],
            recv_sem=recv_c.at[slot], device_id=device, device_id_type=MESH,
        )

    others = range(1, members)
    for i in others:
        spread(i).start()
    arrived[member] = parts[member]
    outs = [
        pltpu.make_async_copy(yw.at[:, own], y_any, out_sems.at[0]),
        pltpu.make_async_copy(z, z_any, out_sems.at[1]),
    ]
    for out in outs:
        out.start()
    for i in others:
        spread(i, True).wait_recv()
    along[layer] = jnp.sum(arrived[...], axis=0)
    pl.semaphore_wait(from_low.at[last], 1)
    for k in range(depth // 2, depth - stages[last]):
        over(k - 1).start()
    pl.semaphore_wait(from_high.at[last], 1)
    for k in range(depth // 2 - 1, 0, -1):
        over(k - 1).start()
        if k < stages[last]:
            over(depth - k - 1).start()
    over(depth - stages[last] - 1).start()
    x_finish()
    p_finish()
    y_finish()
    for out in outs:
        out.wait()
    for i in others:
        spread(i).wait_send()
    each(depth - 1, lambda k: over(k, True).wait_recv())
    gathered[member] = jnp.sum(along[...], axis=0)
    for i in others:
        share(i).start()
    each(depth - 1, lambda k: over(k).wait_send())
    for i in others:
        share(i, True).wait_recv()
    total_ref[...] = gathered[...]
    for i in others:
        share(i).wait_send()


def eliminated(matrix):
    n, lanes = matrix.shape
    block = 16
    pieces = [matrix[i : i + block] for i in range(0, n, block)]
    done = []
    for b in range(n // block):
        rest = jnp.concatenate(pieces[b:], axis=0) if b < n // block - 1 else pieces[b]
        tall = rest.shape[0]
        row = lax.broadcasted_iota(jnp.int32, (tall, lanes), 0)
        columns = [
            jnp.broadcast_to(rest[:, b * block + j : b * block + j + 1], (tall, lanes))
            for j in range(block)
        ]
        pivots = jnp.ones((block, lanes), F32)
        for j in range(block):
            pivot = columns[j][j : j + 1]
            inverse = 1.0 / pivot
            pivots = jnp.where(row[:block] == j, pivot, pivots)
            below = jnp.where(row > j, columns[j], 0.0)
            rest = rest - below * (rest[j : j + 1] * inverse)
            for i in range(j + 1, block):
                columns[i] = columns[i] - below * (columns[i][j : j + 1] * inverse)
        pieces[b:] = [rest[i : i + block] for i in range(0, tall, block)]
        done.append(pieces[b] * lax.rsqrt(pivots))
    return jnp.concatenate(done, axis=0) if len(done) > 1 else done[0]


def precise(left, right, turned=False):
    return lax.dot_general(
        left, right, (((1,), (1 if turned else 0,)), ((), ())),
        precision=lax.Precision.HIGHEST, preferred_element_type=F32,
    )


def three_products(left, right):
    rows = left.shape[0]
    high, low = halves(left)
    top, bottom = halves(right)
    out = jnp.dot(jnp.concatenate([high, low], axis=0), top, preferred_element_type=F32)
    return out[:rows] + (out[rows:] + jnp.dot(high, bottom, preferred_element_type=F32))


def dense_kernel(
    vertex_total, total_ref, x_any, y_any, z_any, locked_any, w_any, image_any, ritz,
    xs, ys, zs, w, image, locked_s, sems,
):
    channels = xs.shape[0]
    loads = [
        pltpu.make_async_copy(source, target, sems.at[i])
        for i, (source, target) in enumerate(
            ((locked_any, locked_s), (x_any, xs), (y_any, ys), (z_any, zs))
        )
    ]
    for load in loads:
        load.start()
    packed = jnp.concatenate([total_ref[i] for i in range(total_ref.shape[0])], axis=0)
    first, folded = packed[:channels], packed[channels:]

    def part(v, i):
        return v[:, i * channels : (i + 1) * channels]

    xx, xy, xp, xq, xz, pp, pq, pz = (part(first, i) for i in range(8))
    second = jnp.concatenate([folded, pltpu.roll(folded, 64, 1)], axis=0)
    yy, yp = part(second, 1), part(second, 2)
    shape = (channels, channels)
    row = lax.broadcasted_iota(jnp.int32, shape, 0)
    column = lax.broadcasted_iota(jnp.int32, shape, 1)
    eye = jnp.where(row == column, 1.0, 0.0).astype(F32)
    yx = xy.T
    top = eye * (xy + 1e-06)
    below = eye * (xx + 1e-06)
    c_down = jnp.sum(top, axis=1, keepdims=True) / jnp.sum(below, axis=1, keepdims=True)
    c_along = jnp.sum(top, axis=0, keepdims=True) / jnp.sum(below, axis=0, keepdims=True)
    loads[0].wait()
    locked = locked_s[0]
    free_down = (lax.broadcasted_iota(jnp.int32, (channels, 1), 0) >= locked).astype(F32)
    free_along = (lax.broadcasted_iota(jnp.int32, (1, channels), 1) >= locked).astype(F32)
    scale = 1.0 / vertex_total
    frozen = eye * (1.0 - free_down)
    rx = free_down * (c_down * xx - yx)
    ry = free_down * (c_down * xy - yy)
    gram_w = free_along * (rx * c_along - ry) * scale + frozen
    inverse = eliminated(jnp.concatenate([gram_w, eye], axis=1))[:, channels:]

    lane = lax.broadcasted_iota(jnp.int32, first.shape, 1)
    rd = jnp.where(lane < channels, jnp.concatenate([rx] * 8, axis=1), free_down * (c_down * first - second))
    wd = precise(inverse, rd)
    wx, wy, wp, wq, wz = (part(wd, i) for i in range(5))
    px, py = xp.T, yp.T

    def against_r(vx, vy):
        return free_along * (vx * c_along - vy)

    def against_image(vx, vy, vz):
        return free_along * (c_along * (vx - vy) - vy + vz)

    stacked = jnp.concatenate(
        [against_r(wx, wy), against_image(xx, xy, xz), against_image(wx, wy, wz),
         against_image(px, py, pz)], axis=0,
    )
    stacked = precise(stacked, inverse, turned=True)
    ww, xaw, waw, paw = (stacked[i * channels : (i + 1) * channels] for i in range(4))

    for load in loads[1:]:
        load.wait()
    r = free_down * (c_down * xs[...] - ys[...])
    nr = free_down * (c_down * ys[...] - zs[...])
    w[...] = three_products(inverse, r)
    image[...] = three_products(inverse, r - nr)
    stores = [
        pltpu.make_async_copy(w, w_any, sems.at[4]),
        pltpu.make_async_copy(image, image_any, sems.at[5]),
    ]
    for store in stores:
        store.start()

    gram_b = jnp.concatenate(
        [
            jnp.concatenate([xx, wx.T, xp], axis=1) * scale,
            jnp.concatenate([wx * scale, ww * scale + frozen, wp * scale], axis=1),
            jnp.concatenate([px, wp.T, pp], axis=1) * scale,
        ], axis=0,
    )
    gram_a = jnp.concatenate(
        [
            jnp.concatenate([xx - xy, xaw, xp - xq], axis=1),
            jnp.concatenate([wx - wy, waw, wp - wq], axis=1),
            jnp.concatenate([px - py, paw, pp - pq], axis=1),
        ], axis=0,
    ) * scale
    n = 3 * channels
    big = (
        lax.broadcasted_iota(jnp.int32, (n, n), 0) == lax.broadcasted_iota(jnp.int32, (n, n), 1)
    ).astype(F32)
    lower = eliminated(jnp.concatenate([gram_b, big], axis=1))[:, n:]
    symmetric = 0.5 * (gram_a + gram_a.T)
    ritz[...] = precise(precise(lower, symmetric), lower, turned=True)
    for store in stores:
        store.wait()


def body(sizes, current_block, previous_block, adjacency_tiles, tile_rows, tile_cols, tile_count, locked):
    channels, here = current_block.shape
    slots, width, _ = adjacency_tiles.shape
    depth, cols, sub = sizes
    members = cols * sub
    rows_each = PACKED // members
    span = 2 * here // width
    vmem = pl.BlockSpec(memory_space=pltpu.VMEM)
    anywhere = pl.BlockSpec(memory_space=pltpu.HBM)
    dma = pltpu.SemaphoreType.DMA
    regular = pltpu.SemaphoreType.REGULAR
    i32 = jnp.int32

    def like(*shape):
        return jax.ShapeDtypeStruct(shape, F32)

    total, y, z = pl.pallas_call(
        functools.partial(main_kernel, sizes),
        name="main",
        out_shape=(pltpu.VMEM((members, rows_each, 128), F32), like(channels, here), like(channels, here)),
        in_specs=[anywhere] * 6,
        out_specs=(vmem, anywhere, anywhere),
        scratch_shapes=[
            VMEM((channels, 2 * here), F32),
            VMEM((channels, 2 * here), F32),
            VMEM((channels, 2 * here), F32),
            VMEM((span, 2 * channels, width), BF16),
            VMEM((span, 2 * channels, width), BF16),
            VMEM((span, 2 * channels, width), BF16),
            VMEM((slots, width, width), F32),
            VMEM((slots, width, 2 * width), BF16),
            VMEM((slots, channels, width), F32),
            VMEM((channels, here), F32),
            VMEM((channels, here), F32),
            VMEM((members, rows_each, 128), F32),
            VMEM((members, rows_each, 128), F32),
            VMEM((depth, rows_each, 128), F32),
            VMEM((members, rows_each, 128), F32),
            pltpu.SMEM((slots,), i32), pltpu.SMEM((slots,), i32),
            pltpu.SMEM((1,), i32), pltpu.SMEM((slots,), i32),
            dma((5,)), dma((CHUNKS,)), dma((6,)), dma((6,)),
            dma((members,)), dma((members,)),
            dma((depth,)), dma((depth,)),
            dma((members,)), dma((members,)),
            dma((2,)), regular((4,)), regular((4,)), VMEM((3 * channels, 128), F32),
        ],
        compiler_params=pltpu.CompilerParams(collective_id=0, has_side_effects=True),
    )(current_block, previous_block, adjacency_tiles, tile_rows, tile_cols, tile_count)
    return pl.pallas_call(
        functools.partial(dense_kernel, float(here * depth * members)),
        name="dense",
        out_shape=(like(channels, here), like(channels, here), like(3 * channels, 3 * channels)),
        in_specs=[vmem] + [anywhere] * 4,
        out_specs=(anywhere, anywhere, vmem),
        scratch_shapes=[VMEM((channels, here), F32)] * 5
        + [pltpu.SMEM((1,), i32), dma((6,))],
    )(pltpu.with_memory_space_constraint(total, pltpu.VMEM), current_block, y, z, locked)


def solution(mesh):
    sizes = tuple(mesh.shape[a] for a in VERTEX_AXES)
    everywhere = ("graphs", "rows", "cols", "sub")
    in_specs = (
        P(None, everywhere),
        P(None, everywhere),
        P(everywhere, None, None),
        P(everywhere),
        P(everywhere),
        P(everywhere),
        P("graphs"),
    )
    out_specs = (P(None, everywhere), P(None, everywhere), P("graphs", None))
    return jax.shard_map(
        functools.partial(body, sizes), mesh=mesh, in_specs=in_specs, out_specs=out_specs,
        check_vma=False,
    )
```

```python
import functools

import jax
import jax.numpy as jnp
from jax import lax
from jax.experimental import pallas as pl
from jax.experimental.pallas import tpu as pltpu
from jax.sharding import PartitionSpec as P

MESH = pl.DeviceIdType.MESH
F32 = jnp.float32
BF16 = jnp.bfloat16
VMEM = pltpu.VMEM
VERTEX_AXES = ("rows", "cols", "sub")
CHUNKS = 4
GROUP = 8
PACKED = 24


def halves(value):
    high = value.astype(BF16)
    return high, (value - high.astype(F32)).astype(BF16)


def tile_copies(tiles_ref, tiles, sems):
    each = tiles.shape[0] // CHUNKS
    return [
        pltpu.make_async_copy(
            tiles_ref.at[pl.ds(i * each, each)], tiles.at[pl.ds(i * each, each)], sems.at[i]
        )
        for i in range(CHUNKS)
    ]


def fill_tiles(split, first, value):
    width = split.shape[2]
    for i in range(value.shape[1] // width):
        split[first + i] = jnp.concatenate(halves(value[:, i * width : (i + 1) * width]), axis=0)


def split_tiles(tiles, pairs, first, last):
    def step(block, carry):
        for lane in range(GROUP // 2):
            slot = block * (GROUP // 2) + lane
            pairs[slot] = jnp.concatenate(halves(tiles[slot]), axis=1)
        return carry

    lax.fori_loop(first // (GROUP // 2), last // (GROUP // 2), step, 0)


def products(split, pairs, prods, first, last, column):
    width = pairs.shape[1]
    channels = split.shape[1] // 2

    def step(block, carry):
        for lane in range(GROUP):
            slot = block * GROUP + lane
            out = jnp.dot(split[column(slot)], pairs[slot], preferred_element_type=F32)
            top, bottom = out[:channels], out[channels:]
            prods[slot] = (
                top[:, :width] + (top[:, width:] + bottom[:, :width])
            ) + bottom[:, width:]
        return carry

    lax.fori_loop(first // GROUP, last // GROUP, step, 0)


def summed_rows(prods, codes, row_tiles, store, after=None):
    slots, channels, width = prods.shape
    size = row_tiles // 2
    for block in range(2):
        mine = [block * size + i for i in range(size)]

        def step(slot, sums):
            value = prods[slot]
            row = jnp.full((channels, width), codes[slot], jnp.int32)
            return tuple(s + jnp.where(row == i, value, 0.0) for i, s in zip(mine, sums))

        sums = lax.fori_loop(
            row_tiles, slots, step, tuple(prods[i] for i in mine), unroll=4
        )
        for i, s in zip(mine, sums):
            store(i, s)
        if after is not None:
            after[block]()


def place(sizes):
    rows, cols, sub = (lax.axis_index(a) for a in VERTEX_AXES)
    return (rows * sizes[1] + cols) * sizes[2] + sub


def device_at(position, sizes):
    return {
        "rows": lax.div(position, sizes[1] * sizes[2]),
        "cols": lax.rem(lax.div(position, sizes[2]), sizes[1]),
        "sub": lax.rem(position, sizes[2]),
    }


def main_kernel(
    sizes, x_any, p_any, tiles_any, rows_any, cols_any, count_any, total_ref, y_any, z_any,
    xw, pw, yw, sx, sp, sy, tiles, pairs, prods, q, z, parts, arrived, along, gathered,
    rows_s, cols_s, count_s, codes, load_sems, tile_sems, halo_send, halo_recv,
    send_a, recv_a, send_b, recv_b, send_c, recv_c, out_sems, from_low, from_high, ring_low, ring_high, gram_s,
):
    channels, here = q.shape
    slots, width, _ = tiles.shape
    row_tiles = here // width
    reach = here // 2
    reach_tiles = reach // width
    depth, cols, sub = sizes
    members = cols * sub
    total = depth * members
    me = place(sizes)
    base = me * row_tiles
    layer = lax.axis_index("rows")
    member = lax.axis_index("cols") * sub + lax.axis_index("sub")
    near = max(1, depth // 16)
    stages = [near]
    while 2 * stages[-1] < depth // 2:
        stages.append(2 * stages[-1])
    own = pl.ds(reach, here)
    low_side, high_side = pl.ds(0, reach), pl.ds(reach + here, reach)

    def layer_by(offset):
        other = layer + offset
        other = jnp.where(other >= depth, other - depth, other)
        return jnp.where(other < 0, other + depth, other)

    def layer_at(k):
        return layer_by(k + 1)

    def member_by(offset):
        other = member + offset
        other = jnp.where(other >= members, other - members, other)
        other = jnp.where(other < 0, other + members, other)
        return other, {"cols": lax.div(other, sub), "sub": lax.rem(other, sub)}

    def each(n, act):
        def step(k, carry):
            act(k)
            return carry

        lax.fori_loop(0, n, step, 0)

    def tell(stage):
        greet(from_low.at[stage], {"rows": layer_by(stages[stage])})
        greet(from_high.at[stage], {"rows": layer_by(-stages[stage])})

    def hear(stage):
        pl.semaphore_wait(from_low.at[stage], 1)
        pl.semaphore_wait(from_high.at[stage], 1)

    rings = []
    while members > 1 and 2 ** len(rings) < members // 2:
        rings.append(2 ** len(rings))

    def tell_members(stage):
        greet(ring_low.at[stage], member_by(rings[stage])[1])
        greet(ring_high.at[stage], member_by(-rings[stage])[1])

    def hear_members(stage):
        pl.semaphore_wait(ring_low.at[stage], 1)
        pl.semaphore_wait(ring_high.at[stage], 1)

    last = len(stages) - 1
    barrier = pltpu.get_barrier_semaphore()

    def greet(semaphore, device):
        pl.semaphore_signal(semaphore, inc=1, device_id=device, device_id_type=MESH)

    has_low, has_high = me > 0, me < total - 1
    low = device_at(jnp.maximum(me - 1, 0), sizes)
    high = device_at(jnp.minimum(me + 1, total - 1), sizes)

    load_x = pltpu.make_async_copy(x_any, xw.at[:, own], load_sems.at[0])
    load_x.start()

    @pl.when(has_low)
    def _():
        greet(barrier, low)

    @pl.when(has_high)
    def _():
        greet(barrier, high)

    adjacent = 2 if members > 1 else 0
    for offset in (1, -1)[:adjacent]:
        greet(barrier, member_by(offset)[1])
    for offset in range(1, near + 1):
        greet(barrier, {"rows": layer_by(offset)})
        greet(barrier, {"rows": layer_by(-offset)})
    load_p = pltpu.make_async_copy(p_any, pw.at[:, own], load_sems.at[1])
    small = [
        pltpu.make_async_copy(source, target, load_sems.at[2 + i])
        for i, (source, target) in enumerate(
            ((rows_any, rows_s), (cols_any, cols_s), (count_any, count_s))
        )
    ]
    loads = tile_copies(tiles_any, tiles, tile_sems)
    for load in [load_p, *small, *loads]:
        load.start()
    pl.semaphore_wait(
        barrier,
        has_low.astype(jnp.int32) + has_high.astype(jnp.int32) + (adjacent + 2 * near),
    )

    def halo(wide, n):
        def remote(source, target, k, device):
            return pltpu.make_async_remote_copy(
                src_ref=wide.at[:, source], dst_ref=wide.at[:, target],
                send_sem=halo_send.at[k], recv_sem=halo_recv.at[k],
                device_id=device, device_id_type=MESH,
            )

        down = remote(pl.ds(reach, reach), high_side, 2 * n, low)
        up = remote(pl.ds(here, reach), low_side, 2 * n + 1, high)

        def start_down():
            @pl.when(has_low)
            def _():
                down.start()

        def start_up():
            @pl.when(has_high)
            def _():
                up.start()

        def arrive():
            @pl.when(has_low)
            def _():
                up.wait_recv()

            @pl.when(has_high)
            def _():
                down.wait_recv()

        def finish():
            @pl.when(has_low)
            def _():
                down.wait_send()

            @pl.when(has_high)
            def _():
                up.wait_send()

        return (start_down, start_up), arrive, finish

    x_start, x_arrive, x_finish = halo(xw, 0)
    p_start, p_arrive, p_finish = halo(pw, 1)
    y_start, y_arrive, y_finish = halo(yw, 2)

    if rings:
        tell_members(0)
    load_x.wait()
    for start in x_start:
        start()
    load_p.wait()
    for start in p_start:
        start()
    tell(0)

    @pl.when(jnp.logical_not(has_low))
    def _():
        for wide in (xw, pw, yw):
            wide[:, low_side] = jnp.zeros((channels, reach), F32)

    @pl.when(jnp.logical_not(has_high))
    def _():
        for wide in (xw, pw, yw):
            wide[:, high_side] = jnp.zeros((channels, reach), F32)

    for load in small:
        load.wait()
    count = count_s[0]

    def code(slot):
        codes[slot] = jnp.where(slot < count, rows_s[slot] - base, -1)

    each(slots, code)

    def column(slot):
        return jnp.clip(cols_s[slot] - (base - reach_tiles), 0, 2 * row_tiles - 1)

    def inner(split):
        products(split, pairs, prods, 0, row_tiles, lambda slot: slot + reach_tiles)

    def outer(split):
        products(split, pairs, prods, row_tiles, slots, column)

    def fill_own(split, wide):
        fill_tiles(split, reach_tiles, wide[:, own])

    def fill_sides(split, wide):
        fill_tiles(split, 0, wide[:, low_side])
        fill_tiles(split, reach_tiles + row_tiles, wide[:, high_side])

    fill_own(sx, xw)
    for i, load in enumerate(loads):
        load.wait()
        split_tiles(tiles, pairs, i * slots // CHUNKS, (i + 1) * slots // CHUNKS)
    inner(sx)
    for stage in range(1, len(rings)):
        hear_members(stage - 1)
        tell_members(stage)
    for stage in range(last - 1):
        hear(stage)
        tell(stage + 1)
    x_arrive()
    fill_sides(sx, xw)
    outer(sx)

    def store_y(i, value):
        yw[:, pl.ds(reach + i * width, width)] = value

    summed_rows(prods, codes, row_tiles, store_y, y_start)

    fill_own(sp, pw)
    inner(sp)
    p_arrive()
    fill_sides(sp, pw)
    outer(sp)

    def store_q(i, value):
        q[:, pl.ds(i * width, width)] = value

    summed_rows(prods, codes, row_tiles, store_q)

    hear(last - 1)
    tell(last)

    fill_own(sy, yw)
    inner(sy)

    def gram_of(right):
        left = jnp.concatenate([xw[:, own], yw[:, own], pw[:, own]], axis=0)
        return lax.dot_general(
            left, right, (((1,), (1,)), ((), ())), precision=lax.Precision.HIGHEST,
            preferred_element_type=F32,
        )

    gram_s[...] = gram_of(
        jnp.concatenate(
            [xw[:, own], yw[:, own], pw[:, own], q[...], jnp.zeros((4 * channels, here), F32)],
            axis=0,
        )
    )
    y_arrive()
    fill_sides(sy, yw)
    outer(sy)

    def store_z(i, value):
        z[:, pl.ds(i * width, width)] = value

    summed_rows(prods, codes, row_tiles, store_z)
    with_z = gram_of(z[...])
    with_z = jnp.concatenate([with_z, jnp.zeros((3 * channels, 128 - channels), F32)], axis=1)
    gram = gram_s[...] + pltpu.roll(with_z, 4 * channels, 1)
    gram_x, gram_y, gram_p = (gram[i * channels : (i + 1) * channels] for i in range(3))
    lane = lax.broadcasted_iota(jnp.int32, (channels, 128), 1)
    first = jnp.where(lane < 5 * channels, gram_x, pltpu.roll(gram_p, 3 * channels, 1))
    half = channels // 2
    lane = lax.broadcasted_iota(jnp.int32, (half, 128), 1)
    second = jnp.where(
        jnp.logical_and(lane >= channels, lane < 5 * channels),
        gram_y[:half], pltpu.roll(gram_y[half:], 64, 1),
    )
    packed = jnp.concatenate([first, second], axis=0)
    rows_each = PACKED // members
    for i in range(members):
        parts[i] = packed[i * rows_each : (i + 1) * rows_each]

    def spread(offset, incoming=False):
        other, device = member_by(offset)
        slot = other if incoming else member
        return pltpu.make_async_remote_copy(
            src_ref=parts.at[other], dst_ref=arrived.at[slot], send_sem=send_a.at[other],
            recv_sem=recv_a.at[slot], device_id=device, device_id_type=MESH,
        )

    def over(k, incoming=False):
        other = layer_at(k)
        slot = other if incoming else layer
        return pltpu.make_async_remote_copy(
            src_ref=along.at[layer], dst_ref=along.at[slot], send_sem=send_b.at[other],
            recv_sem=recv_b.at[slot], device_id={"rows": other}, device_id_type=MESH,
        )

    def share(offset, incoming=False):
        other, device = member_by(offset)
        slot = other if incoming else member
        return pltpu.make_async_remote_copy(
            src_ref=gathered.at[member], dst_ref=gathered.at[slot], send_sem=send_c.at[other],
            recv_sem=recv_c.at[slot], device_id=device, device_id_type=MESH,
        )

    others = range(1, members)
    if rings:
        hear_members(len(rings) - 1)
    for i in others:
        spread(i).start()
    arrived[member] = parts[member]
    outs = [
        pltpu.make_async_copy(yw.at[:, own], y_any, out_sems.at[0]),
        pltpu.make_async_copy(z, z_any, out_sems.at[1]),
    ]
    for out in outs:
        out.start()
    for i in others:
        spread(i, True).wait_recv()
    along[layer] = jnp.sum(arrived[...], axis=0)
    pl.semaphore_wait(from_low.at[last], 1)
    for k in range(depth // 2, depth - stages[last]):
        over(k - 1).start()
    pl.semaphore_wait(from_high.at[last], 1)
    for k in range(depth // 2 - 1, 0, -1):
        over(k - 1).start()
        if k < stages[last]:
            over(depth - k - 1).start()
    over(depth - stages[last] - 1).start()
    x_finish()
    p_finish()
    y_finish()
    for out in outs:
        out.wait()
    for i in others:
        spread(i).wait_send()
    each(depth - 1, lambda k: over(k, True).wait_recv())
    gathered[member] = jnp.sum(along[...], axis=0)
    for i in others:
        share(i).start()
    each(depth - 1, lambda k: over(k).wait_send())
    for i in others:
        share(i, True).wait_recv()
    total_ref[...] = gathered[...]
    for i in others:
        share(i).wait_send()


def eliminated(matrix):
    n, lanes = matrix.shape
    block = 16
    pieces = [matrix[i : i + block] for i in range(0, n, block)]
    done = []
    for b in range(n // block):
        rest = jnp.concatenate(pieces[b:], axis=0) if b < n // block - 1 else pieces[b]
        tall = rest.shape[0]
        row = lax.broadcasted_iota(jnp.int32, (tall, lanes), 0)
        columns = [
            jnp.broadcast_to(rest[:, b * block + j : b * block + j + 1], (tall, lanes))
            for j in range(block)
        ]
        pivots = jnp.ones((block, lanes), F32)
        for j in range(block):
            pivot = columns[j][j : j + 1]
            inverse = 1.0 / pivot
            pivots = jnp.where(row[:block] == j, pivot, pivots)
            below = jnp.where(row > j, columns[j], 0.0)
            rest = rest - below * (rest[j : j + 1] * inverse)
            for i in range(j + 1, block):
                columns[i] = columns[i] - below * (columns[i][j : j + 1] * inverse)
        pieces[b:] = [rest[i : i + block] for i in range(0, tall, block)]
        done.append(pieces[b] * lax.rsqrt(pivots))
    return jnp.concatenate(done, axis=0) if len(done) > 1 else done[0]


def precise(left, right, turned=False):
    return lax.dot_general(
        left, right, (((1,), (1 if turned else 0,)), ((), ())),
        precision=lax.Precision.HIGHEST, preferred_element_type=F32,
    )


def three_products(left, right):
    rows = left.shape[0]
    high, low = halves(left)
    top, bottom = halves(right)
    out = jnp.dot(jnp.concatenate([high, low], axis=0), top, preferred_element_type=F32)
    return out[:rows] + (out[rows:] + jnp.dot(high, bottom, preferred_element_type=F32))


def dense_kernel(
    vertex_total, total_ref, x_any, y_any, z_any, locked_any, w_any, image_any, ritz,
    xs, ys, zs, w, image, locked_s, sems,
):
    channels = xs.shape[0]
    loads = [
        pltpu.make_async_copy(source, target, sems.at[i])
        for i, (source, target) in enumerate(
            ((locked_any, locked_s), (x_any, xs), (y_any, ys), (z_any, zs))
        )
    ]
    for load in loads:
        load.start()
    packed = jnp.concatenate([total_ref[i] for i in range(total_ref.shape[0])], axis=0)
    first, folded = packed[:channels], packed[channels:]

    def part(v, i):
        return v[:, i * channels : (i + 1) * channels]

    xx, xy, xp, xq, xz, pp, pq, pz = (part(first, i) for i in range(8))
    second = jnp.concatenate([folded, pltpu.roll(folded, 64, 1)], axis=0)
    yy, yp = part(second, 1), part(second, 2)
    shape = (channels, channels)
    row = lax.broadcasted_iota(jnp.int32, shape, 0)
    column = lax.broadcasted_iota(jnp.int32, shape, 1)
    eye = jnp.where(row == column, 1.0, 0.0).astype(F32)
    yx = xy.T
    top = eye * (xy + 1e-06)
    below = eye * (xx + 1e-06)
    c_down = jnp.sum(top, axis=1, keepdims=True) / jnp.sum(below, axis=1, keepdims=True)
    c_along = jnp.sum(top, axis=0, keepdims=True) / jnp.sum(below, axis=0, keepdims=True)
    loads[0].wait()
    locked = locked_s[0]
    free_down = (lax.broadcasted_iota(jnp.int32, (channels, 1), 0) >= locked).astype(F32)
    free_along = (lax.broadcasted_iota(jnp.int32, (1, channels), 1) >= locked).astype(F32)
    scale = 1.0 / vertex_total
    frozen = eye * (1.0 - free_down)
    rx = free_down * (c_down * xx - yx)
    ry = free_down * (c_down * xy - yy)
    gram_w = free_along * (rx * c_along - ry) * scale + frozen
    inverse = eliminated(jnp.concatenate([gram_w, eye], axis=1))[:, channels:]

    lane = lax.broadcasted_iota(jnp.int32, first.shape, 1)
    rd = jnp.where(lane < channels, jnp.concatenate([rx] * 8, axis=1), free_down * (c_down * first - second))
    wd = precise(inverse, rd)
    wx, wy, wp, wq, wz = (part(wd, i) for i in range(5))
    px, py = xp.T, yp.T

    def against_r(vx, vy):
        return free_along * (vx * c_along - vy)

    def against_image(vx, vy, vz):
        return free_along * (c_along * (vx - vy) - vy + vz)

    stacked = jnp.concatenate(
        [against_r(wx, wy), against_image(xx, xy, xz), against_image(wx, wy, wz),
         against_image(px, py, pz)], axis=0,
    )
    stacked = precise(stacked, inverse, turned=True)
    ww, xaw, waw, paw = (stacked[i * channels : (i + 1) * channels] for i in range(4))

    for load in loads[1:]:
        load.wait()
    r = free_down * (c_down * xs[...] - ys[...])
    nr = free_down * (c_down * ys[...] - zs[...])
    w[...] = three_products(inverse, r)
    image[...] = three_products(inverse, r - nr)
    gram_b = jnp.concatenate(
        [
            jnp.concatenate([xx, wx.T, xp], axis=1) * scale,
            jnp.concatenate([wx * scale, ww * scale + frozen, wp * scale], axis=1),
            jnp.concatenate([px, wp.T, pp], axis=1) * scale,
        ], axis=0,
    )
    gram_a = jnp.concatenate(
        [
            jnp.concatenate([xx - xy, xaw, xp - xq], axis=1),
            jnp.concatenate([wx - wy, waw, wp - wq], axis=1),
            jnp.concatenate([px - py, paw, pp - pq], axis=1),
        ], axis=0,
    ) * scale
    n = 3 * channels
    big = (
        lax.broadcasted_iota(jnp.int32, (n, n), 0) == lax.broadcasted_iota(jnp.int32, (n, n), 1)
    ).astype(F32)
    lower = eliminated(jnp.concatenate([gram_b, big], axis=1))[:, n:]
    stores = [
        pltpu.make_async_copy(w, w_any, sems.at[4]),
        pltpu.make_async_copy(image, image_any, sems.at[5]),
    ]
    for store in stores:
        store.start()

    symmetric = 0.5 * (gram_a + gram_a.T)
    ritz[...] = precise(precise(lower, symmetric), lower, turned=True)
    for store in stores:
        store.wait()


def body(sizes, current_block, previous_block, adjacency_tiles, tile_rows, tile_cols, tile_count, locked):
    channels, here = current_block.shape
    slots, width, _ = adjacency_tiles.shape
    depth, cols, sub = sizes
    members = cols * sub
    rows_each = PACKED // members
    span = 2 * here // width
    vmem = pl.BlockSpec(memory_space=pltpu.VMEM)
    anywhere = pl.BlockSpec(memory_space=pltpu.HBM)
    dma = pltpu.SemaphoreType.DMA
    regular = pltpu.SemaphoreType.REGULAR
    i32 = jnp.int32

    def like(*shape):
        return jax.ShapeDtypeStruct(shape, F32)

    total, y, z = pl.pallas_call(
        functools.partial(main_kernel, sizes),
        name="main",
        out_shape=(pltpu.VMEM((members, rows_each, 128), F32), like(channels, here), like(channels, here)),
        in_specs=[anywhere] * 6,
        out_specs=(vmem, anywhere, anywhere),
        scratch_shapes=[
            VMEM((channels, 2 * here), F32),
            VMEM((channels, 2 * here), F32),
            VMEM((channels, 2 * here), F32),
            VMEM((span, 2 * channels, width), BF16),
            VMEM((span, 2 * channels, width), BF16),
            VMEM((span, 2 * channels, width), BF16),
            VMEM((slots, width, width), F32),
            VMEM((slots, width, 2 * width), BF16),
            VMEM((slots, channels, width), F32),
            VMEM((channels, here), F32),
            VMEM((channels, here), F32),
            VMEM((members, rows_each, 128), F32),
            VMEM((members, rows_each, 128), F32),
            VMEM((depth, rows_each, 128), F32),
            VMEM((members, rows_each, 128), F32),
            pltpu.SMEM((slots,), i32), pltpu.SMEM((slots,), i32),
            pltpu.SMEM((1,), i32), pltpu.SMEM((slots,), i32),
            dma((5,)), dma((CHUNKS,)), dma((6,)), dma((6,)),
            dma((members,)), dma((members,)),
            dma((depth,)), dma((depth,)),
            dma((members,)), dma((members,)),
            dma((2,)), regular((4,)), regular((4,)), regular((4,)), regular((4,)), VMEM((3 * channels, 128), F32),
        ],
        compiler_params=pltpu.CompilerParams(collective_id=0, has_side_effects=True),
    )(current_block, previous_block, adjacency_tiles, tile_rows, tile_cols, tile_count)
    return pl.pallas_call(
        functools.partial(dense_kernel, float(here * depth * members)),
        name="dense",
        out_shape=(like(channels, here), like(channels, here), like(3 * channels, 3 * channels)),
        in_specs=[vmem] + [anywhere] * 4,
        out_specs=(anywhere, anywhere, vmem),
        scratch_shapes=[VMEM((channels, here), F32)] * 5
        + [pltpu.SMEM((1,), i32), dma((6,))],
    )(pltpu.with_memory_space_constraint(total, pltpu.VMEM), current_block, y, z, locked)


def solution(mesh):
    sizes = tuple(mesh.shape[a] for a in VERTEX_AXES)
    everywhere = ("graphs", "rows", "cols", "sub")
    in_specs = (
        P(None, everywhere),
        P(None, everywhere),
        P(everywhere, None, None),
        P(everywhere),
        P(everywhere),
        P(everywhere),
        P("graphs"),
    )
    out_specs = (P(None, everywhere), P(None, everywhere), P("graphs", None))
    return jax.shard_map(
        functools.partial(body, sizes), mesh=mesh, in_specs=in_specs, out_specs=out_specs,
        check_vma=False,
    )
```

```python
import functools

import jax
import jax.numpy as jnp
from jax import lax
from jax.experimental import pallas as pl
from jax.experimental.pallas import tpu as pltpu
from jax.sharding import PartitionSpec as P

MESH = pl.DeviceIdType.MESH
F32 = jnp.float32
BF16 = jnp.bfloat16
VMEM = pltpu.VMEM
VERTEX_AXES = ("rows", "cols", "sub")
CHUNKS = 4
GROUP = 8
PACKED = 24


def halves(value):
    high = value.astype(BF16)
    return high, (value - high.astype(F32)).astype(BF16)


def tile_copies(tiles_ref, tiles, sems):
    each = tiles.shape[0] // CHUNKS
    return [
        pltpu.make_async_copy(
            tiles_ref.at[pl.ds(i * each, each)], tiles.at[pl.ds(i * each, each)], sems.at[i]
        )
        for i in range(CHUNKS)
    ]


def fill_tiles(split, first, value):
    width = split.shape[2]
    for i in range(value.shape[1] // width):
        split[first + i] = jnp.concatenate(halves(value[:, i * width : (i + 1) * width]), axis=0)


def split_tiles(tiles, pairs, first, last):
    def step(block, carry):
        for lane in range(GROUP // 2):
            slot = block * (GROUP // 2) + lane
            pairs[slot] = jnp.concatenate(halves(tiles[slot]), axis=1)
        return carry

    lax.fori_loop(first // (GROUP // 2), last // (GROUP // 2), step, 0)


def products(split, pairs, prods, first, last, column):
    width = pairs.shape[1]
    channels = split.shape[1] // 2

    def step(block, carry):
        for lane in range(GROUP):
            slot = block * GROUP + lane
            out = jnp.dot(split[column(slot)], pairs[slot], preferred_element_type=F32)
            top, bottom = out[:channels], out[channels:]
            prods[slot] = (
                top[:, :width] + (top[:, width:] + bottom[:, :width])
            ) + bottom[:, width:]
        return carry

    lax.fori_loop(first // GROUP, last // GROUP, step, 0)


def summed_rows(prods, codes, row_tiles, store, after=None):
    slots, channels, width = prods.shape
    size = row_tiles // 2
    for block in range(2):
        mine = [block * size + i for i in range(size)]

        def step(slot, sums):
            value = prods[slot]
            row = jnp.full((channels, width), codes[slot], jnp.int32)
            return tuple(s + jnp.where(row == i, value, 0.0) for i, s in zip(mine, sums))

        sums = lax.fori_loop(
            row_tiles, slots, step, tuple(prods[i] for i in mine), unroll=4
        )
        for i, s in zip(mine, sums):
            store(i, s)
        if after is not None:
            after[block]()


def place(sizes):
    rows, cols, sub = (lax.axis_index(a) for a in VERTEX_AXES)
    return (rows * sizes[1] + cols) * sizes[2] + sub


def device_at(position, sizes):
    return {
        "rows": lax.div(position, sizes[1] * sizes[2]),
        "cols": lax.rem(lax.div(position, sizes[2]), sizes[1]),
        "sub": lax.rem(position, sizes[2]),
    }


def main_kernel(
    sizes, x_any, p_any, tiles_any, rows_any, cols_any, count_any, total_ref, y_any, z_any,
    xw, pw, yw, sx, sp, sy, tiles, pairs, prods, q, z, parts, arrived, along, gathered,
    rows_s, cols_s, count_s, codes, load_sems, tile_sems, halo_send, halo_recv,
    send_a, recv_a, send_b, recv_b, send_c, recv_c, out_sems, from_low, from_high, ring_low, ring_high, gram_s,
):
    channels, here = q.shape
    slots, width, _ = tiles.shape
    row_tiles = here // width
    reach = here // 2
    reach_tiles = reach // width
    depth, cols, sub = sizes
    members = cols * sub
    total = depth * members
    me = place(sizes)
    base = me * row_tiles
    layer = lax.axis_index("rows")
    member = lax.axis_index("cols") * sub + lax.axis_index("sub")
    near = max(1, depth // 16)
    stages = [near]
    while 2 * stages[-1] < depth // 2:
        stages.append(2 * stages[-1])
    own = pl.ds(reach, here)
    low_side, high_side = pl.ds(0, reach), pl.ds(reach + here, reach)

    def layer_by(offset):
        other = layer + offset
        other = jnp.where(other >= depth, other - depth, other)
        return jnp.where(other < 0, other + depth, other)

    def layer_at(k):
        return layer_by(k + 1)

    def member_by(offset):
        other = member + offset
        other = jnp.where(other >= members, other - members, other)
        other = jnp.where(other < 0, other + members, other)
        return other, {"cols": lax.div(other, sub), "sub": lax.rem(other, sub)}

    def each(n, act):
        def step(k, carry):
            act(k)
            return carry

        lax.fori_loop(0, n, step, 0)

    def tell(stage):
        greet(from_low.at[stage], {"rows": layer_by(stages[stage])})
        greet(from_high.at[stage], {"rows": layer_by(-stages[stage])})

    def hear(stage):
        pl.semaphore_wait(from_low.at[stage], 1)
        pl.semaphore_wait(from_high.at[stage], 1)

    rings = []
    while members > 1 and 2 ** len(rings) < members // 2:
        rings.append(2 ** len(rings))

    def tell_members(stage):
        greet(ring_low.at[stage], member_by(rings[stage])[1])
        greet(ring_high.at[stage], member_by(-rings[stage])[1])

    def hear_members(stage):
        pl.semaphore_wait(ring_low.at[stage], 1)
        pl.semaphore_wait(ring_high.at[stage], 1)

    last = len(stages) - 1
    barrier = pltpu.get_barrier_semaphore()

    def greet(semaphore, device):
        pl.semaphore_signal(semaphore, inc=1, device_id=device, device_id_type=MESH)

    has_low, has_high = me > 0, me < total - 1
    low = device_at(jnp.maximum(me - 1, 0), sizes)
    high = device_at(jnp.minimum(me + 1, total - 1), sizes)

    load_x = pltpu.make_async_copy(x_any, xw.at[:, own], load_sems.at[0])
    load_x.start()

    @pl.when(has_low)
    def _():
        greet(barrier, low)

    @pl.when(has_high)
    def _():
        greet(barrier, high)

    adjacent = 2 if members > 1 else 0
    for offset in (1, -1)[:adjacent]:
        greet(barrier, member_by(offset)[1])
    for offset in range(1, near + 1):
        greet(barrier, {"rows": layer_by(offset)})
        greet(barrier, {"rows": layer_by(-offset)})
    load_p = pltpu.make_async_copy(p_any, pw.at[:, own], load_sems.at[1])
    small = [
        pltpu.make_async_copy(source, target, load_sems.at[2 + i])
        for i, (source, target) in enumerate(
            ((rows_any, rows_s), (cols_any, cols_s), (count_any, count_s))
        )
    ]
    loads = tile_copies(tiles_any, tiles, tile_sems)
    for load in [load_p, *small, *loads]:
        load.start()
    pl.semaphore_wait(
        barrier,
        has_low.astype(jnp.int32) + has_high.astype(jnp.int32) + (adjacent + 2 * near),
    )

    def halo(wide, n):
        def remote(source, target, k, device):
            return pltpu.make_async_remote_copy(
                src_ref=wide.at[:, source], dst_ref=wide.at[:, target],
                send_sem=halo_send.at[k], recv_sem=halo_recv.at[k],
                device_id=device, device_id_type=MESH,
            )

        down = remote(pl.ds(reach, reach), high_side, 2 * n, low)
        up = remote(pl.ds(here, reach), low_side, 2 * n + 1, high)

        def start_down():
            @pl.when(has_low)
            def _():
                down.start()

        def start_up():
            @pl.when(has_high)
            def _():
                up.start()

        def arrive():
            @pl.when(has_low)
            def _():
                up.wait_recv()

            @pl.when(has_high)
            def _():
                down.wait_recv()

        def finish():
            @pl.when(has_low)
            def _():
                down.wait_send()

            @pl.when(has_high)
            def _():
                up.wait_send()

        return (start_down, start_up), arrive, finish

    x_start, x_arrive, x_finish = halo(xw, 0)
    p_start, p_arrive, p_finish = halo(pw, 1)
    y_start, y_arrive, y_finish = halo(yw, 2)

    if rings:
        tell_members(0)
    load_x.wait()
    for start in x_start:
        start()
    load_p.wait()
    for start in p_start:
        start()
    tell(0)

    @pl.when(jnp.logical_not(has_low))
    def _():
        for wide in (xw, pw, yw):
            wide[:, low_side] = jnp.zeros((channels, reach), F32)

    @pl.when(jnp.logical_not(has_high))
    def _():
        for wide in (xw, pw, yw):
            wide[:, high_side] = jnp.zeros((channels, reach), F32)

    for load in small:
        load.wait()
    count = count_s[0]

    def code(slot):
        codes[slot] = jnp.where(slot < count, rows_s[slot] - base, -1)

    each(slots, code)

    def column(slot):
        return jnp.clip(cols_s[slot] - (base - reach_tiles), 0, 2 * row_tiles - 1)

    def inner(split):
        products(split, pairs, prods, 0, row_tiles, lambda slot: slot + reach_tiles)

    def outer(split):
        products(split, pairs, prods, row_tiles, slots, column)

    def fill_own(split, wide):
        fill_tiles(split, reach_tiles, wide[:, own])

    def fill_sides(split, wide):
        fill_tiles(split, 0, wide[:, low_side])
        fill_tiles(split, reach_tiles + row_tiles, wide[:, high_side])

    fill_own(sx, xw)
    for i, load in enumerate(loads):
        load.wait()
        split_tiles(tiles, pairs, i * slots // CHUNKS, (i + 1) * slots // CHUNKS)
    inner(sx)
    for stage in range(1, len(rings)):
        hear_members(stage - 1)
        tell_members(stage)
    for stage in range(last - 1):
        hear(stage)
        tell(stage + 1)
    x_arrive()
    fill_sides(sx, xw)
    outer(sx)

    def store_y(i, value):
        yw[:, pl.ds(reach + i * width, width)] = value

    summed_rows(prods, codes, row_tiles, store_y, y_start)

    fill_own(sp, pw)
    inner(sp)
    p_arrive()
    fill_sides(sp, pw)
    outer(sp)

    def store_q(i, value):
        q[:, pl.ds(i * width, width)] = value

    summed_rows(prods, codes, row_tiles, store_q)

    fill_own(sy, yw)
    inner(sy)
    hear(last - 1)
    tell(last)

    def gram_of(right):
        left = jnp.concatenate([xw[:, own], yw[:, own], pw[:, own]], axis=0)
        return lax.dot_general(
            left, right, (((1,), (1,)), ((), ())), precision=lax.Precision.HIGHEST,
            preferred_element_type=F32,
        )

    gram_s[...] = gram_of(
        jnp.concatenate(
            [xw[:, own], yw[:, own], pw[:, own], q[...], jnp.zeros((4 * channels, here), F32)],
            axis=0,
        )
    )
    y_arrive()
    fill_sides(sy, yw)
    outer(sy)

    def store_z(i, value):
        z[:, pl.ds(i * width, width)] = value

    summed_rows(prods, codes, row_tiles, store_z)
    with_z = gram_of(z[...])
    with_z = jnp.concatenate([with_z, jnp.zeros((3 * channels, 128 - channels), F32)], axis=1)
    gram = gram_s[...] + pltpu.roll(with_z, 4 * channels, 1)
    gram_x, gram_y, gram_p = (gram[i * channels : (i + 1) * channels] for i in range(3))
    lane = lax.broadcasted_iota(jnp.int32, (channels, 128), 1)
    first = jnp.where(lane < 5 * channels, gram_x, pltpu.roll(gram_p, 3 * channels, 1))
    half = channels // 2
    lane = lax.broadcasted_iota(jnp.int32, (half, 128), 1)
    second = jnp.where(
        jnp.logical_and(lane >= channels, lane < 5 * channels),
        gram_y[:half], pltpu.roll(gram_y[half:], 64, 1),
    )
    packed = jnp.concatenate([first, second], axis=0)
    rows_each = PACKED // members
    for i in range(members):
        parts[i] = packed[i * rows_each : (i + 1) * rows_each]

    def spread(offset, incoming=False):
        other, device = member_by(offset)
        slot = other if incoming else member
        return pltpu.make_async_remote_copy(
            src_ref=parts.at[other], dst_ref=arrived.at[slot], send_sem=send_a.at[other],
            recv_sem=recv_a.at[slot], device_id=device, device_id_type=MESH,
        )

    def over(k, incoming=False):
        other = layer_at(k)
        slot = other if incoming else layer
        return pltpu.make_async_remote_copy(
            src_ref=along.at[layer], dst_ref=along.at[slot], send_sem=send_b.at[other],
            recv_sem=recv_b.at[slot], device_id={"rows": other}, device_id_type=MESH,
        )

    def share(offset, incoming=False):
        other, device = member_by(offset)
        slot = other if incoming else member
        return pltpu.make_async_remote_copy(
            src_ref=gathered.at[member], dst_ref=gathered.at[slot], send_sem=send_c.at[other],
            recv_sem=recv_c.at[slot], device_id=device, device_id_type=MESH,
        )

    others = range(1, members)
    if rings:
        hear_members(len(rings) - 1)
    for i in others:
        spread(i).start()
    arrived[member] = parts[member]
    outs = [
        pltpu.make_async_copy(yw.at[:, own], y_any, out_sems.at[0]),
        pltpu.make_async_copy(z, z_any, out_sems.at[1]),
    ]
    for out in outs:
        out.start()
    for i in others:
        spread(i, True).wait_recv()
    along[layer] = jnp.sum(arrived[...], axis=0)
    pl.semaphore_wait(from_low.at[last], 1)
    for k in range(depth // 2, depth - stages[last]):
        over(k - 1).start()
    pl.semaphore_wait(from_high.at[last], 1)
    for k in range(depth // 2 - 1, 0, -1):
        over(k - 1).start()
        if k < stages[last]:
            over(depth - k - 1).start()
    over(depth - stages[last] - 1).start()
    x_finish()
    p_finish()
    y_finish()
    for out in outs:
        out.wait()
    for i in others:
        spread(i).wait_send()
    each(depth - 1, lambda k: over(k, True).wait_recv())
    gathered[member] = jnp.sum(along[...], axis=0)
    for i in others:
        share(i).start()
    each(depth - 1, lambda k: over(k).wait_send())
    for i in others:
        share(i, True).wait_recv()
    total_ref[...] = gathered[...]
    for i in others:
        share(i).wait_send()


def eliminated(matrix):
    n, lanes = matrix.shape
    block = 16
    pieces = [matrix[i : i + block] for i in range(0, n, block)]
    done = []
    for b in range(n // block):
        rest = jnp.concatenate(pieces[b:], axis=0) if b < n // block - 1 else pieces[b]
        tall = rest.shape[0]
        row = lax.broadcasted_iota(jnp.int32, (tall, lanes), 0)
        columns = [
            jnp.broadcast_to(rest[:, b * block + j : b * block + j + 1], (tall, lanes))
            for j in range(block)
        ]
        pivots = jnp.ones((block, lanes), F32)
        for j in range(block):
            pivot = columns[j][j : j + 1]
            inverse = 1.0 / pivot
            pivots = jnp.where(row[:block] == j, pivot, pivots)
            below = jnp.where(row > j, columns[j], 0.0)
            rest = rest - below * (rest[j : j + 1] * inverse)
            for i in range(j + 1, block):
                columns[i] = columns[i] - below * (columns[i][j : j + 1] * inverse)
        pieces[b:] = [rest[i : i + block] for i in range(0, tall, block)]
        done.append(pieces[b] * lax.rsqrt(pivots))
    return jnp.concatenate(done, axis=0) if len(done) > 1 else done[0]


def precise(left, right, turned=False):
    return lax.dot_general(
        left, right, (((1,), (1 if turned else 0,)), ((), ())),
        precision=lax.Precision.HIGHEST, preferred_element_type=F32,
    )


def three_products(left, right):
    rows = left.shape[0]
    high, low = halves(left)
    top, bottom = halves(right)
    out = jnp.dot(jnp.concatenate([high, low], axis=0), top, preferred_element_type=F32)
    return out[:rows] + (out[rows:] + jnp.dot(high, bottom, preferred_element_type=F32))


def dense_kernel(
    vertex_total, total_ref, x_any, y_any, z_any, locked_any, w_any, image_any, ritz,
    xs, ys, zs, w, image, locked_s, sems,
):
    channels = xs.shape[0]
    loads = [
        pltpu.make_async_copy(source, target, sems.at[i])
        for i, (source, target) in enumerate(
            ((locked_any, locked_s), (x_any, xs), (y_any, ys), (z_any, zs))
        )
    ]
    for load in loads:
        load.start()
    packed = jnp.concatenate([total_ref[i] for i in range(total_ref.shape[0])], axis=0)
    first, folded = packed[:channels], packed[channels:]

    def part(v, i):
        return v[:, i * channels : (i + 1) * channels]

    xx, xy, xp, xq, xz, pp, pq, pz = (part(first, i) for i in range(8))
    second = jnp.concatenate([folded, pltpu.roll(folded, 64, 1)], axis=0)
    yy, yp = part(second, 1), part(second, 2)
    shape = (channels, channels)
    row = lax.broadcasted_iota(jnp.int32, shape, 0)
    column = lax.broadcasted_iota(jnp.int32, shape, 1)
    eye = jnp.where(row == column, 1.0, 0.0).astype(F32)
    yx = xy.T
    top = eye * (xy + 1e-06)
    below = eye * (xx + 1e-06)
    c_down = jnp.sum(top, axis=1, keepdims=True) / jnp.sum(below, axis=1, keepdims=True)
    c_along = jnp.sum(top, axis=0, keepdims=True) / jnp.sum(below, axis=0, keepdims=True)
    loads[0].wait()
    locked = locked_s[0]
    free_down = (lax.broadcasted_iota(jnp.int32, (channels, 1), 0) >= locked).astype(F32)
    free_along = (lax.broadcasted_iota(jnp.int32, (1, channels), 1) >= locked).astype(F32)
    scale = 1.0 / vertex_total
    frozen = eye * (1.0 - free_down)
    rx = free_down * (c_down * xx - yx)
    ry = free_down * (c_down * xy - yy)
    gram_w = free_along * (rx * c_along - ry) * scale + frozen
    inverse = eliminated(jnp.concatenate([gram_w, eye], axis=1))[:, channels:]

    lane = lax.broadcasted_iota(jnp.int32, first.shape, 1)
    rd = jnp.where(lane < channels, jnp.concatenate([rx] * 8, axis=1), free_down * (c_down * first - second))
    wd = precise(inverse, rd)
    wx, wy, wp, wq, wz = (part(wd, i) for i in range(5))
    px, py = xp.T, yp.T

    def against_r(vx, vy):
        return free_along * (vx * c_along - vy)

    def against_image(vx, vy, vz):
        return free_along * (c_along * (vx - vy) - vy + vz)

    stacked = jnp.concatenate(
        [against_r(wx, wy), against_image(xx, xy, xz), against_image(wx, wy, wz),
         against_image(px, py, pz)], axis=0,
    )
    stacked = precise(stacked, inverse, turned=True)
    ww, xaw, waw, paw = (stacked[i * channels : (i + 1) * channels] for i in range(4))

    for load in loads[1:]:
        load.wait()
    r = free_down * (c_down * xs[...] - ys[...])
    nr = free_down * (c_down * ys[...] - zs[...])
    w[...] = three_products(inverse, r)
    image[...] = three_products(inverse, r - nr)
    gram_b = jnp.concatenate(
        [
            jnp.concatenate([xx, wx.T, xp], axis=1) * scale,
            jnp.concatenate([wx * scale, ww * scale + frozen, wp * scale], axis=1),
            jnp.concatenate([px, wp.T, pp], axis=1) * scale,
        ], axis=0,
    )
    gram_a = jnp.concatenate(
        [
            jnp.concatenate([xx - xy, xaw, xp - xq], axis=1),
            jnp.concatenate([wx - wy, waw, wp - wq], axis=1),
            jnp.concatenate([px - py, paw, pp - pq], axis=1),
        ], axis=0,
    ) * scale
    n = 3 * channels
    big = (
        lax.broadcasted_iota(jnp.int32, (n, n), 0) == lax.broadcasted_iota(jnp.int32, (n, n), 1)
    ).astype(F32)
    lower = eliminated(jnp.concatenate([gram_b, big], axis=1))[:, n:]
    stores = [
        pltpu.make_async_copy(w, w_any, sems.at[4]),
        pltpu.make_async_copy(image, image_any, sems.at[5]),
    ]
    for store in stores:
        store.start()

    symmetric = 0.5 * (gram_a + gram_a.T)
    ritz[...] = precise(precise(lower, symmetric), lower, turned=True)
    for store in stores:
        store.wait()


def body(sizes, current_block, previous_block, adjacency_tiles, tile_rows, tile_cols, tile_count, locked):
    channels, here = current_block.shape
    slots, width, _ = adjacency_tiles.shape
    depth, cols, sub = sizes
    members = cols * sub
    rows_each = PACKED // members
    span = 2 * here // width
    vmem = pl.BlockSpec(memory_space=pltpu.VMEM)
    anywhere = pl.BlockSpec(memory_space=pltpu.HBM)
    dma = pltpu.SemaphoreType.DMA
    regular = pltpu.SemaphoreType.REGULAR
    i32 = jnp.int32

    def like(*shape):
        return jax.ShapeDtypeStruct(shape, F32)

    total, y, z = pl.pallas_call(
        functools.partial(main_kernel, sizes),
        name="main",
        out_shape=(pltpu.VMEM((members, rows_each, 128), F32), like(channels, here), like(channels, here)),
        in_specs=[anywhere] * 6,
        out_specs=(vmem, anywhere, anywhere),
        scratch_shapes=[
            VMEM((channels, 2 * here), F32),
            VMEM((channels, 2 * here), F32),
            VMEM((channels, 2 * here), F32),
            VMEM((span, 2 * channels, width), BF16),
            VMEM((span, 2 * channels, width), BF16),
            VMEM((span, 2 * channels, width), BF16),
            VMEM((slots, width, width), F32),
            VMEM((slots, width, 2 * width), BF16),
            VMEM((slots, channels, width), F32),
            VMEM((channels, here), F32),
            VMEM((channels, here), F32),
            VMEM((members, rows_each, 128), F32),
            VMEM((members, rows_each, 128), F32),
            VMEM((depth, rows_each, 128), F32),
            VMEM((members, rows_each, 128), F32),
            pltpu.SMEM((slots,), i32), pltpu.SMEM((slots,), i32),
            pltpu.SMEM((1,), i32), pltpu.SMEM((slots,), i32),
            dma((5,)), dma((CHUNKS,)), dma((6,)), dma((6,)),
            dma((members,)), dma((members,)),
            dma((depth,)), dma((depth,)),
            dma((members,)), dma((members,)),
            dma((2,)), regular((4,)), regular((4,)), regular((4,)), regular((4,)), VMEM((3 * channels, 128), F32),
        ],
        compiler_params=pltpu.CompilerParams(collective_id=0, has_side_effects=True),
    )(current_block, previous_block, adjacency_tiles, tile_rows, tile_cols, tile_count)
    return pl.pallas_call(
        functools.partial(dense_kernel, float(here * depth * members)),
        name="dense",
        out_shape=(like(channels, here), like(channels, here), like(3 * channels, 3 * channels)),
        in_specs=[vmem] + [anywhere] * 4,
        out_specs=(anywhere, anywhere, vmem),
        scratch_shapes=[VMEM((channels, here), F32)] * 5
        + [pltpu.SMEM((1,), i32), dma((6,))],
    )(pltpu.with_memory_space_constraint(total, pltpu.VMEM), current_block, y, z, locked)


def solution(mesh):
    sizes = tuple(mesh.shape[a] for a in VERTEX_AXES)
    everywhere = ("graphs", "rows", "cols", "sub")
    in_specs = (
        P(None, everywhere),
        P(None, everywhere),
        P(everywhere, None, None),
        P(everywhere),
        P(everywhere),
        P(everywhere),
        P("graphs"),
    )
    out_specs = (P(None, everywhere), P(None, everywhere), P("graphs", None))
    return jax.shard_map(
        functools.partial(body, sizes), mesh=mesh, in_specs=in_specs, out_specs=out_specs,
        check_vma=False,
    )
```
